512 devices in a mesh: parts: 2 (over y), tile: 128 (over x, z), cond: 2 (over core).
Axes of the slice: x: 8, y: 2, z: 16, core: 2. Of those that a mesh axis runs over, the one named last changes fastest.
The devices are a block of a 8x8x16 slice.
Arguments:
- mask: bfloat16 [256, 256, 256], P(('parts', 'tile')), parts along dimension 0, may hold values from -1 to 1
- kernels: bfloat16 [8, 24, 64, 128], P('cond'), may hold values from -6 to 6
- socs_weight: float32 [8, 24], P('cond'), may hold values from 0.02 to 1
- dose: float32 [8], P('cond'), may hold values from 0.8 to 1.25
- threshold: float32 [8], P('cond'), may hold values from 0.5 to 0.85
Outputs:
- band_max: float32 [256, 256, 256], P(('parts', 'tile'), 'cond'), parts along dimension 0
- band_min: float32 [256, 256, 256], P(('parts', 'tile'), 'cond'), parts along dimension 0
The draws below stay inside these ranges and needn't reach their ends.
There are 2 independent parts, one for each index of `parts`. The reference program is written for one: setup_inputs(seed, part) draws one part's arguments, and reference() takes and returns one part's arrays. A program takes and returns all parts, laid end to end along the dimension named above; an argument that names none is the same for every part. Nothing has to cross between parts.
All inputs are finite; a program needn't handle non-finite values.
Results may differ from the reference program's by a relative error of at most 0.0068.
Values may be sent and summed in bfloat16 or wider, within the bound.
A program may use at most 64 MiB of HBM per device.

```python
import math
import jax
import jax.numpy as jnp
from jax import lax

CORE = 256
MARGIN = 64
BLUR = 8
BAND = 64
KERN = 24
COND = 8
TILES = 128
N_TILE = 128


def levels(own_key, shape, split, smallest, largest):
    def one(dim, shards_of):
        heights = jax.random.uniform(jax.random.fold_in(jax.random.fold_in(own_key, 6), dim), (shards_of,), jnp.float32, smallest / len(split), largest / len(split))
        return jnp.repeat(jnp.exp(heights), shape[dim] // shards_of).reshape((-1,) + (1,) * (len(shape) - dim - 1))

    factor_of = one(*split[0])
    for cut in split[1:]:
        factor_of = factor_of * one(*cut)
    return factor_of


def normal_values(stream_key, shape, scale, bound, cuts=(), held_as=jnp.bfloat16):
    loudness = levels(stream_key, shape, cuts, -0.22, 0.18) if cuts else 1.0
    array = jax.random.normal(stream_key, shape, jnp.float32) * scale * loudness
    return jnp.minimum(jnp.maximum(array, -bound), bound).astype(held_as)


def setup_inputs(seed: int = 0, part: int = 0) -> dict:
    key_of = jax.random.split(jax.random.key(seed), 6)
    own_keys = jax.random.split(jax.random.fold_in(key_of[5], part), 6)
    mask = jnp.clip(jax.random.uniform(own_keys[0], (TILES, CORE, CORE), jnp.float32, -1.0, 1.0) * levels(own_keys[0], (TILES, CORE, CORE), ((0, 128),), -0.4, 0.0), -1.0, 1.0).astype(jnp.bfloat16)
    kernels = normal_values(key_of[1], (COND, KERN, BAND, 2 * BAND), 1.0, 6.0, ((0, 2),))
    socs_weight = jnp.clip(jnp.exp(math.log(1.0) - 3.912023 * jax.random.uniform(key_of[2], (COND, KERN), jnp.float32) ** levels(key_of[2], (COND, KERN), ((0, 2),), -0.2, 0.2)), 0.02, 1.0)
    dose = jnp.clip(0.8 + 0.45 * jax.random.uniform(key_of[3], (COND,), jnp.float32) ** levels(key_of[3], (COND,), ((0, 2),), -0.2, 0.2), 0.8, 1.25)
    threshold = jnp.clip(0.5 + 0.35000002 * jax.random.uniform(key_of[4], (COND,), jnp.float32) ** levels(key_of[4], (COND,), ((0, 2),), -0.2, 0.2), 0.5, 0.85)
    return dict(mask=mask, kernels=kernels, socs_weight=socs_weight, dose=dose, threshold=threshold)


diffusion = 2.0
steepness = 8.0


def phase_table(first, count, pad_width, band_width):
    pixel_index = jnp.arange(count, dtype=jnp.int32) + first
    freq_index = (jnp.arange(band_width, dtype=jnp.int32) - band_width // 2) % pad_width
    turn_count = (pixel_index[:, None] * freq_index[None, :]) % pad_width
    angle_grid = turn_count.astype(jnp.float32) * (2.0 * math.pi / pad_width)
    return jnp.cos(angle_grid).astype(jnp.bfloat16), jnp.sin(angle_grid).astype(jnp.bfloat16)


def blur_table(core):
    offset_grid = jnp.arange(core + 2 * BLUR, dtype=jnp.int32)[None, :] - jnp.arange(core, dtype=jnp.int32)[:, None] - BLUR
    distance = offset_grid.astype(jnp.float32)
    taps_grid = jnp.exp(-distance * distance / (2.0 * diffusion * diffusion))
    taps_grid = jnp.where(jnp.abs(offset_grid) <= BLUR, taps_grid, jnp.zeros_like(taps_grid))
    reach_grid = jnp.arange(-BLUR, BLUR + 1, dtype=jnp.int32).astype(jnp.float32)
    total_taps = jnp.sum(jnp.exp(-reach_grid * reach_grid / (2.0 * diffusion * diffusion)))
    return taps_grid / total_taps


def make_tables(core, band_width):
    pad_width = core + 2 * MARGIN
    cos_in, sin_in = phase_table(0, pad_width, pad_width, band_width)
    cos_out, sin_out = phase_table(MARGIN - BLUR, core + 2 * BLUR, pad_width, band_width)
    return cos_in, sin_in, cos_out, sin_out, blur_table(core)


def expose(window, kernel_set, weights, dose_one, threshold_one, tables):
    cos_in, sin_in, cos_out, sin_out, blur_rows = tables
    pad_width = window.shape[0]
    band_width = cos_in.shape[1]
    hp = lax.Precision.HIGHEST
    part_real = jnp.dot(cos_in.T, window, preferred_element_type=jnp.float32).astype(jnp.bfloat16)
    part_imag = (-jnp.dot(sin_in.T, window, preferred_element_type=jnp.float32)).astype(jnp.bfloat16)
    spec_real = (jnp.dot(part_real, cos_in, preferred_element_type=jnp.float32) + jnp.dot(part_imag, sin_in, preferred_element_type=jnp.float32)) / pad_width
    spec_imag = (jnp.dot(part_imag, cos_in, preferred_element_type=jnp.float32) - jnp.dot(part_real, sin_in, preferred_element_type=jnp.float32)) / pad_width
    group_size = min(8, kernel_set.shape[0])
    kernel_groups = kernel_set.reshape(-1, group_size, band_width, 2 * band_width)
    weight_groups = weights.reshape(-1, group_size)
    cos_wide = cos_out.astype(jnp.float32)
    sin_wide = sin_out.astype(jnp.float32)

    def group_power(packed):
        kernel_part, weight_part = packed
        kern_real = kernel_part[:, :, :band_width].astype(jnp.float32)
        kern_imag = kernel_part[:, :, band_width:].astype(jnp.float32)
        prod_real = (spec_real * kern_real - spec_imag * kern_imag).astype(jnp.bfloat16).astype(jnp.float32)
        prod_imag = (spec_real * kern_imag + spec_imag * kern_real).astype(jnp.bfloat16).astype(jnp.float32)
        half_real = (jnp.einsum('nfg,yg->nfy', prod_real, cos_wide, precision=hp) - jnp.einsum('nfg,yg->nfy', prod_imag, sin_wide, precision=hp)).astype(jnp.bfloat16).astype(jnp.float32)
        half_imag = (jnp.einsum('nfg,yg->nfy', prod_real, sin_wide, precision=hp) + jnp.einsum('nfg,yg->nfy', prod_imag, cos_wide, precision=hp)).astype(jnp.bfloat16).astype(jnp.float32)
        field_real = (jnp.einsum('xf,nfy->nxy', cos_wide, half_real, precision=hp) - jnp.einsum('xf,nfy->nxy', sin_wide, half_imag, precision=hp)) / band_width
        field_imag = (jnp.einsum('xf,nfy->nxy', cos_wide, half_imag, precision=hp) + jnp.einsum('xf,nfy->nxy', sin_wide, half_real, precision=hp)) / band_width
        power = field_real * field_real + field_imag * field_imag
        return jnp.tensordot(weight_part, power, axes=1, precision=hp)

    intensity = jnp.sum(lax.map(group_power, (kernel_groups, weight_groups)), axis=0) / jnp.sum(weights)
    blurred = jnp.dot(jnp.dot(blur_rows, intensity, precision=hp), blur_rows.T, precision=hp)
    return jax.nn.sigmoid(steepness * (dose_one * blurred - threshold_one))


def reference(mask, kernels, socs_weight, dose, threshold):
    count = mask.shape[0]
    core = mask.shape[1]
    columns = min(8, N_TILE // 2)
    grid_rows = count // columns
    rotate = columns // 2
    holder = (jnp.arange(count, dtype=jnp.int32) - rotate) % count
    placed = mask[holder]
    region_plane = placed.reshape(grid_rows, columns, core, core).transpose(0, 2, 1, 3).reshape(grid_rows * core, columns * core)
    padded = jnp.pad(region_plane, MARGIN)
    tables = make_tables(core, kernels.shape[2])
    pad_width = core + 2 * MARGIN

    def one_tile(index):
        position = (index + rotate) % count
        top_row = ((position // columns) * core).astype(jnp.int32)
        left_col = ((position % columns) * core).astype(jnp.int32)
        window = lax.dynamic_slice(padded, (top_row, left_col), (pad_width, pad_width))

        def one_condition(packed):
            kernel_set, weights, dose_one, threshold_one = packed
            return expose(window, kernel_set, weights, dose_one, threshold_one, tables)

        resist = lax.map(one_condition, (kernels, socs_weight, dose, threshold))
        return jnp.max(resist, axis=0), jnp.min(resist, axis=0)

    highest, lowest = lax.map(one_tile, jnp.arange(count, dtype=jnp.int32))
    return highest, lowest
```

```python
import functools

import jax
import jax.numpy as jnp
import numpy as np
from jax import lax
from jax.experimental import pallas as pl
from jax.experimental.pallas import tpu as pltpu
from jax.sharding import PartitionSpec as P

MESH = pl.DeviceIdType.MESH
MARGIN = 64
BLUR = 8
LANES = 128
STEP = 3
PACK = 4

diffusion = 2.0
steepness = 8.0


def phase(pixels, pad_width, band_width):
    freq = np.arange(band_width) - band_width // 2
    angle = 2.0 * np.pi * ((pixels[:, None] * freq[None, :]) % pad_width) / pad_width
    return np.cos(angle), np.sin(angle)


def make_tables(core, band_width):
    pad_width = core + 2 * MARGIN
    bf16 = lambda a: np.asarray(a, np.float32).astype(jnp.bfloat16)
    cos_in, sin_in = phase(np.arange(pad_width), pad_width, band_width)
    both = np.concatenate([cos_in, -sin_in], axis=1)
    gap = np.zeros((LANES - MARGIN, 2 * band_width))
    columns = np.concatenate([gap, both, gap], axis=0)
    rows = np.concatenate([cos_in.T, sin_in.T], axis=0)
    own_rows = rows[:, MARGIN : MARGIN + core]
    far_rows = np.concatenate([rows[:, :MARGIN], rows[:, MARGIN + core :]], axis=1)
    count = pad_width // STEP
    cos_s, sin_s = phase(np.arange(count) * STEP, pad_width, band_width)
    first = np.block([[cos_s, -sin_s, -sin_s, cos_s], [sin_s, cos_s, cos_s, sin_s]])
    nil = np.zeros((band_width, count))
    second = np.block(
        [
            [cos_s.T, sin_s.T, nil, nil],
            [nil, nil, cos_s.T, sin_s.T],
            [-sin_s.T, cos_s.T, nil, nil],
            [nil, nil, -sin_s.T, cos_s.T],
        ]
    )
    offset = np.arange(core + 2 * BLUR)[None, :] - np.arange(core)[:, None] - BLUR
    taps = np.where(np.abs(offset) <= BLUR, np.exp(-(offset**2) / (2.0 * diffusion**2)), 0.0)
    reach = np.arange(-BLUR, BLUR + 1)
    taps = taps / np.sum(np.exp(-(reach**2) / (2.0 * diffusion**2)))
    pixel = np.arange(MARGIN - BLUR, MARGIN + core + BLUR)
    wave = np.arange(-(band_width - 1), band_width)
    apart = pixel[:, None] - STEP * np.arange(count)[None, :]
    interpolate = np.cos(2.0 * np.pi * apart[:, :, None] * wave / pad_width).sum(-1) / count
    smooth = np.asarray(taps @ interpolate, np.float32)
    high = bf16(smooth).astype(np.float32)
    low = smooth - high
    rows_out = np.concatenate([high, low, high], axis=1)
    cols_out = np.concatenate([high.T, low.T, high.T], axis=0)
    half = core // 2
    rows_out = rows_out.reshape(2, half, 3 * count)
    return tuple(bf16(a) for a in (columns, own_rows, far_rows, first, second, rows_out, cols_out))


def nt_dot(a, b):
    return lax.dot_general(a, b, (((1,), (1,)), ((), ())), preferred_element_type=jnp.float32)


def dot(a, b):
    return jnp.dot(a, b, preferred_element_type=jnp.float32)


def halves(a):
    high = a.astype(jnp.bfloat16)
    return high, (a - high.astype(jnp.float32)).astype(jnp.bfloat16)


def kernel(
    tiles,
    weight_ref,
    dose_ref,
    threshold_ref,
    mask_hbm,
    kernels_hbm,
    columns_hbm,
    own_rows_hbm,
    far_rows_hbm,
    first_hbm,
    second_hbm,
    rows_out_hbm,
    cols_out_hbm,
    high_ref,
    low_ref,
    mask_v,
    kernels_v,
    columns_v,
    own_rows_v,
    far_rows_v,
    first_v,
    second_v,
    rows_out_v,
    cols_out_v,
    left_v,
    right_v,
    spec_rows,
    far_v,
    own_level,
    sib_level,
    load_sem,
    send_sem,
    recv_sem,
    level_send,
    level_recv,
):
    conds, kerns, band = kernels_v.shape[:3]
    core = mask_v.shape[0]
    tile = lax.axis_index("tile")
    cond = lax.axis_index("cond")
    grid_cols = min(8, tiles // 2)
    grid_rows = tiles // grid_cols
    place = lax.rem(tile + grid_cols // 2, tiles)
    column = lax.rem(place, grid_cols)
    row = lax.div(place, grid_cols)
    right = {"tile": lax.rem(tile + 1, tiles)}
    left = {"tile": lax.rem(tile + tiles - 1, tiles)}
    down = {"tile": lax.rem(tile + grid_cols, tiles)}
    up = {"tile": lax.rem(tile + tiles - grid_cols, tiles)}
    sibling = {"cond": 1 - cond}

    barrier = pltpu.get_barrier_semaphore()
    for peer in (up, down, left, right, sibling):
        pl.semaphore_signal(barrier, inc=1, device_id=peer, device_id_type=MESH)

    sources = (
        mask_hbm.at[0],
        columns_hbm,
        own_rows_hbm,
        far_rows_hbm,
        first_hbm,
        second_hbm,
        rows_out_hbm,
        cols_out_hbm,
    )
    targets = (
        mask_v,
        columns_v,
        own_rows_v,
        far_rows_v,
        first_v,
        second_v,
        rows_out_v,
        cols_out_v,
    )
    loads = [
        pltpu.make_async_copy(s, t, load_sem.at[i]) for i, (s, t) in enumerate(zip(sources, targets))
    ]
    for c in range(conds):
        loads.append(
            pltpu.make_async_copy(kernels_hbm.at[c], kernels_v.at[c], load_sem.at[len(sources) + c])
        )
    for load in loads:
        load.start()
    for load in loads:
        load.wait()

    def remote(src, dst, i, peer):
        return pltpu.make_async_remote_copy(
            src_ref=src,
            dst_ref=dst,
            send_sem=send_sem.at[i],
            recv_sem=recv_sem.at[i],
            device_id=peer,
            device_id_type=MESH,
        )

    to_right = remote(mask_v.at[:, core - LANES :], left_v, 0, right)
    to_left = remote(mask_v.at[:, :LANES], right_v, 1, left)
    to_down = remote(spec_rows.at[core - MARGIN :], far_v.at[:MARGIN], 2, down)
    to_up = remote(spec_rows.at[:MARGIN], far_v.at[MARGIN:], 3, up)

    pl.semaphore_wait(barrier, 5)
    to_right.start()
    to_left.start()

    part = dot(mask_v[...], columns_v[LANES : LANES + core])
    to_right.wait_recv()
    zero = jnp.zeros((core, LANES), jnp.bfloat16)
    part += dot(jnp.where(column > 0, left_v[...], zero), columns_v[:LANES])
    to_left.wait_recv()
    part += dot(
        jnp.where(column < grid_cols - 1, right_v[...], zero), columns_v[LANES + core :]
    )
    spec_rows[...] = part.astype(jnp.bfloat16)
    to_down.start()
    to_up.start()
    mixed = dot(own_rows_v[...], spec_rows[...])
    to_down.wait_recv()
    to_up.wait_recv()
    zero = jnp.zeros((MARGIN, 2 * band), jnp.bfloat16)
    above = jnp.where(row > 0, far_v[:MARGIN], zero)
    below = jnp.where(row < grid_rows - 1, far_v[MARGIN:], zero)
    mixed += dot(far_rows_v[...], jnp.concatenate([above, below], axis=0))
    mixed *= 1.0 / ((core + 2 * MARGIN) * band)
    lower = lax.broadcasted_iota(jnp.int32, (band, 2 * band), 1) < band
    turned = pltpu.roll(mixed[band:], band, axis=1)
    spec = mixed[:band] + jnp.where(lower, turned, -turned)
    swapped = pltpu.roll(spec, band, axis=1)
    reals = jnp.where(lower, spec, swapped)
    imags = jnp.where(lower, swapped, -spec)
    spec_one = jnp.concatenate([reals, imags], axis=1)

    count = own_level.shape[1]
    level_copies = []
    for c in range(conds):

        def group(g, level, c=c):
            held = kernels_v[c, pl.ds(g * PACK, PACK)].astype(jnp.float32)
            rows = []
            for j in range(PACK):
                rows.append(
                    (spec_one * jnp.concatenate([held[j], held[j]], axis=1)).astype(jnp.bfloat16)
                )
            packed = jnp.concatenate(rows, axis=0)
            half = nt_dot(first_v[...], packed).astype(jnp.bfloat16)
            for j in range(PACK // 2):
                span = slice(j * 2 * band, (j + 1) * 2 * band)
                pair = jnp.concatenate([half[:count, span], half[count:, span]], axis=1)
                field = dot(pair, second_v[...])
                for i in range(2):
                    re = field[:, 2 * i * count : (2 * i + 1) * count]
                    im = field[:, (2 * i + 1) * count : (2 * i + 2) * count]
                    level += weight_ref[c, g * PACK + 2 * j + i] * (re * re + im * im)
            return level

        level = lax.fori_loop(
            0, kerns // PACK, group, jnp.zeros((count, count), jnp.float32), unroll=True
        )
        total = weight_ref[c, 0]
        for k in range(1, kerns):
            total += weight_ref[c, k]
        scale = jnp.full((1, count), steepness * dose_ref[c]) / jnp.full((1, count), total)
        own_level[c] = level * scale - steepness * threshold_ref[c]
        copy = pltpu.make_async_remote_copy(
            src_ref=own_level.at[c],
            dst_ref=sib_level.at[c],
            send_sem=level_send.at[c],
            recv_sem=level_recv.at[c],
            device_id=sibling,
            device_id_type=MESH,
        )
        copy.start()
        level_copies.append(copy)

    rows_out = rows_out_v[cond]
    high = low = None
    for i in range(2 * conds):
        if i < conds:
            level = own_level[i]
        else:
            level_copies[i - conds].wait_recv()
            level = sib_level[i - conds]
        fine, rest = halves(level)
        tall = nt_dot(rows_out, jnp.concatenate([fine, fine, rest], axis=1))
        fine, rest = halves(tall)
        logit = dot(jnp.concatenate([fine, fine, rest], axis=1), cols_out_v[...])
        high = logit if high is None else jnp.maximum(high, logit)
        low = logit if low is None else jnp.minimum(low, logit)
    high_ref[0] = jax.nn.sigmoid(high)
    low_ref[0] = jax.nn.sigmoid(low)

    for copy in (to_right, to_left, to_down, to_up, *level_copies):
        copy.wait_send()


def on_device(mask, kernels, socs_weight, dose, threshold):
    core = mask.shape[1]
    conds, kerns, band = kernels.shape[:3]
    tables = [jnp.asarray(t) for t in make_tables(core, band)]
    count = (core + 2 * MARGIN) // STEP
    smem = pl.BlockSpec(memory_space=pltpu.SMEM)
    anywhere = pl.BlockSpec(memory_space=pl.ANY)
    vmem = pl.BlockSpec(memory_space=pltpu.VMEM)
    loads = 1 + len(tables) + conds
    out = jax.ShapeDtypeStruct((1, core // 2, core), jnp.float32)
    return pl.pallas_call(
        functools.partial(kernel, lax.axis_size("tile")),
        out_shape=(out, out),
        in_specs=[smem] * 3 + [anywhere] * (2 + len(tables)),
        out_specs=(vmem, vmem),
        scratch_shapes=[
            pltpu.VMEM(mask.shape[1:], mask.dtype),
            pltpu.VMEM(kernels.shape, kernels.dtype),
            *[pltpu.VMEM(t.shape, t.dtype) for t in tables],
            pltpu.VMEM((core, LANES), mask.dtype),
            pltpu.VMEM((core, LANES), mask.dtype),
            pltpu.VMEM((core, 2 * band), jnp.bfloat16),
            pltpu.VMEM((2 * MARGIN, 2 * band), jnp.bfloat16),
            pltpu.VMEM((conds, count, count), jnp.float32),
            pltpu.VMEM((conds, count, count), jnp.float32),
            pltpu.SemaphoreType.DMA((loads,)),
            pltpu.SemaphoreType.DMA((4,)),
            pltpu.SemaphoreType.DMA((4,)),
            pltpu.SemaphoreType.DMA((conds,)),
            pltpu.SemaphoreType.DMA((conds,)),
        ],
        compiler_params=pltpu.CompilerParams(collective_id=0, has_side_effects=True),
        name="expose",
    )(socs_weight, dose, threshold, mask, kernels, *tables)


def solution(mesh):
    return jax.shard_map(
        on_device,
        mesh=mesh,
        in_specs=(
            P(("parts", "tile"), None, None),
            P("cond", None, None, None),
            P("cond", None),
            P("cond"),
            P("cond"),
        ),
        out_specs=(P(("parts", "tile"), "cond", None), P(("parts", "tile"), "cond", None)),
        check_vma=False,
    )
```

```python
import functools

import jax
import jax.numpy as jnp
import numpy as np
from jax import lax
from jax.experimental import pallas as pl
from jax.experimental.pallas import tpu as pltpu
from jax.sharding import PartitionSpec as P

MESH = pl.DeviceIdType.MESH
MARGIN = 64
BLUR = 8
LANES = 128
STEP = 3
PACK = 4
GROUP = 8

diffusion = 2.0
steepness = 8.0


def phase(pixels, pad_width, band_width):
    freq = np.arange(band_width) - band_width // 2
    angle = 2.0 * np.pi * ((pixels[:, None] * freq[None, :]) % pad_width) / pad_width
    return np.cos(angle), np.sin(angle)


def make_tables(core, band_width):
    pad_width = core + 2 * MARGIN
    bf16 = lambda a: np.asarray(a, np.float32).astype(jnp.bfloat16)
    cos_in, sin_in = phase(np.arange(pad_width), pad_width, band_width)
    both = np.concatenate([cos_in, -sin_in], axis=1)
    columns = both[MARGIN : MARGIN + core]
    nil = np.zeros((MARGIN, 2 * band_width))
    strips = []
    for strip in (both[:MARGIN], both[MARGIN + core :]):
        strips.append(np.block([[strip, nil], [nil, strip]]))
    rows = np.concatenate([cos_in.T, sin_in.T], axis=0)
    own_rows = rows[:, MARGIN : MARGIN + core]
    far_rows = np.concatenate([rows[:, :MARGIN], rows[:, MARGIN + core :]], axis=1)
    count = pad_width // STEP
    cos_s, sin_s = phase(np.arange(count) * STEP, pad_width, band_width)
    first = np.block([[cos_s, -sin_s, -sin_s, cos_s], [sin_s, cos_s, cos_s, sin_s]])
    nil = np.zeros((band_width, count))
    second = np.block(
        [
            [cos_s.T, sin_s.T, nil, nil],
            [nil, nil, cos_s.T, sin_s.T],
            [-sin_s.T, cos_s.T, nil, nil],
            [nil, nil, -sin_s.T, cos_s.T],
        ]
    )
    offset = np.arange(core + 2 * BLUR)[None, :] - np.arange(core)[:, None] - BLUR
    taps = np.where(np.abs(offset) <= BLUR, np.exp(-(offset**2) / (2.0 * diffusion**2)), 0.0)
    reach = np.arange(-BLUR, BLUR + 1)
    taps = taps / np.sum(np.exp(-(reach**2) / (2.0 * diffusion**2)))
    pixel = np.arange(MARGIN - BLUR, MARGIN + core + BLUR)
    wave = np.arange(-(band_width - 1), band_width)
    apart = pixel[:, None] - STEP * np.arange(count)[None, :]
    interpolate = np.cos(2.0 * np.pi * apart[:, :, None] * wave / pad_width).sum(-1) / count
    smooth = np.asarray(taps @ interpolate, np.float32)
    high = bf16(smooth).astype(np.float32)
    low = smooth - high
    rows_out = np.concatenate([high, low, high], axis=1)
    cols_out = np.concatenate([high.T, low.T, high.T], axis=0)
    rows_out = rows_out.reshape(2, core // 2, 3 * count)
    return tuple(
        bf16(a) for a in (columns, np.stack(strips), own_rows, far_rows, first, second, rows_out, cols_out)
    )


def nt_dot(a, b):
    return lax.dot_general(a, b, (((1,), (1,)), ((), ())), preferred_element_type=jnp.float32)


def dot(a, b):
    return jnp.dot(a, b, preferred_element_type=jnp.float32)


def halves(a):
    high = a.astype(jnp.bfloat16)
    return high, (a - high.astype(jnp.float32)).astype(jnp.bfloat16)


def spot(tiles):
    grid_cols = min(8, tiles // 2)
    place = lax.rem(lax.axis_index("tile") + grid_cols // 2, tiles)
    column = lax.rem(place, grid_cols)
    row = lax.div(place, grid_cols)
    odd = lax.rem(row, 2) == 1
    seam_left = jnp.logical_and(odd, column == grid_cols // 2)
    seam_right = jnp.logical_and(odd, column == grid_cols // 2 - 1)
    return grid_cols, column, row, seam_left, seam_right


def last_columns(mask_v):
    rows, columns = mask_v.shape
    upper = mask_v[: rows // 2, columns - LANES :].astype(jnp.float32)
    lower = mask_v[rows // 2 :, columns - LANES :].astype(jnp.float32)
    early = lax.broadcasted_iota(jnp.int32, upper.shape, 1) < MARGIN
    return jnp.where(early, pltpu.roll(upper, MARGIN, axis=1), lower).astype(mask_v.dtype)


def first_columns(mask_v):
    rows = mask_v.shape[0]
    upper = mask_v[: rows // 2, :LANES].astype(jnp.float32)
    lower = mask_v[rows // 2 :, :LANES].astype(jnp.float32)
    early = lax.broadcasted_iota(jnp.int32, upper.shape, 1) < MARGIN
    return jnp.where(early, upper, pltpu.roll(lower, MARGIN, axis=1)).astype(mask_v.dtype)


def seam_kernel(tiles, mask_hbm, strip_hbm, mask_v, packed_v, load_sem, send_sem, recv_sem):
    tile = lax.axis_index("tile")
    _, _, _, seam_left, seam_right = spot(tiles)

    def exchange(peer, pack):
        barrier = pltpu.get_barrier_semaphore()
        pl.semaphore_signal(barrier, inc=1, device_id=peer, device_id_type=MESH)
        load = pltpu.make_async_copy(mask_hbm.at[0], mask_v, load_sem)
        load.start()
        load.wait()
        packed_v[...] = pack(mask_v)
        pl.semaphore_wait(barrier, 1)
        copy = pltpu.make_async_remote_copy(
            src_ref=packed_v,
            dst_ref=strip_hbm,
            send_sem=send_sem,
            recv_sem=recv_sem,
            device_id=peer,
            device_id_type=MESH,
        )
        copy.start()
        copy.wait()

    @pl.when(seam_right)
    def _():
        exchange({"tile": lax.rem(tile + 1, tiles)}, last_columns)

    @pl.when(seam_left)
    def _():
        exchange({"tile": lax.rem(tile + tiles - 1, tiles)}, first_columns)


def kernel(
    tiles,
    weight_hbm,
    dose_ref,
    threshold_ref,
    mask_hbm,
    kernels_hbm,
    strip_hbm,
    columns_hbm,
    strips_hbm,
    own_rows_hbm,
    far_rows_hbm,
    first_hbm,
    second_hbm,
    rows_out_hbm,
    cols_out_hbm,
    high_ref,
    low_ref,
    weight_ref,
    mask_v,
    kernels_v,
    columns_v,
    strips_v,
    own_rows_v,
    far_rows_v,
    first_v,
    second_v,
    rows_out_v,
    cols_out_v,
    packed_v,
    left_v,
    right_v,
    spec_rows,
    far_v,
    pair_v,
    own_level,
    sib_level,
    load_sem,
    strip_sem,
    send_sem,
    recv_sem,
    level_send,
    level_recv,
):
    conds, kerns, band = kernels_v.shape[:3]
    core = mask_v.shape[0]
    half = core // 2
    count = own_level.shape[1]
    tile = lax.axis_index("tile")
    cond = lax.axis_index("cond")
    grid_cols, column, row, seam_left, seam_right = spot(tiles)
    has_left = column > 0
    has_right = column < grid_cols - 1
    has_up = row > 0
    has_down = row < tiles // grid_cols - 1
    greet_left = jnp.logical_and(has_left, jnp.logical_not(seam_left))
    greet_right = jnp.logical_and(has_right, jnp.logical_not(seam_right))
    right = {"tile": lax.rem(tile + 1, tiles)}
    left = {"tile": lax.rem(tile + tiles - 1, tiles)}
    down = {"tile": lax.rem(tile + grid_cols, tiles)}
    up = {"tile": lax.rem(tile + tiles - grid_cols, tiles)}
    sibling = {"cond": 1 - cond}

    barrier = pltpu.get_barrier_semaphore()
    peers = 1
    for flag, peer in ((has_up, up), (has_down, down), (greet_left, left), (greet_right, right)):
        peers = peers + flag.astype(jnp.int32)

        @pl.when(flag)
        def _(peer=peer):
            pl.semaphore_signal(barrier, inc=1, device_id=peer, device_id_type=MESH)

    pl.semaphore_signal(barrier, inc=1, device_id=sibling, device_id_type=MESH)

    sources = (
        mask_hbm.at[0],
        columns_hbm,
        strips_hbm,
        own_rows_hbm,
        far_rows_hbm,
        first_hbm,
        second_hbm,
        weight_hbm,
        rows_out_hbm,
        cols_out_hbm,
        *[kernels_hbm.at[c] for c in range(conds)],
    )
    targets = (
        mask_v,
        columns_v,
        strips_v,
        own_rows_v,
        far_rows_v,
        first_v,
        second_v,
        weight_ref,
        rows_out_v,
        cols_out_v,
        *[kernels_v.at[c] for c in range(conds)],
    )
    loads = [
        pltpu.make_async_copy(s, t, load_sem.at[i]) for i, (s, t) in enumerate(zip(sources, targets))
    ]
    for load in loads:
        load.start()
    from_seam = [
        (seam_left, pltpu.make_async_copy(strip_hbm, left_v, strip_sem)),
        (seam_right, pltpu.make_async_copy(strip_hbm, right_v, strip_sem)),
    ]
    for flag, copy in from_seam:
        pl.when(flag)(copy.start)

    def remote(src, dst, i, peer):
        return pltpu.make_async_remote_copy(
            src_ref=src,
            dst_ref=dst,
            send_sem=send_sem.at[i],
            recv_sem=recv_sem.at[i],
            device_id=peer,
            device_id_type=MESH,
        )

    to_right = remote(packed_v.at[0], left_v, 0, right)
    to_left = remote(packed_v.at[1], right_v, 1, left)
    to_down = remote(spec_rows.at[core - MARGIN :], far_v.at[:MARGIN], 2, down)
    to_up = remote(spec_rows.at[:MARGIN], far_v.at[MARGIN:], 3, up)

    loads[0].wait()
    packed_v[0] = last_columns(mask_v)
    packed_v[1] = first_columns(mask_v)
    pl.semaphore_wait(barrier, peers)
    pl.when(greet_right)(to_right.start)
    pl.when(greet_left)(to_left.start)

    for load in loads[1:]:
        load.wait()
    part = dot(mask_v[...], columns_v[...])
    zero = jnp.zeros((half, LANES), jnp.bfloat16)
    pl.when(seam_left)(from_seam[0][1].wait)
    pl.when(seam_right)(from_seam[1][1].wait)
    pl.when(greet_left)(to_right.wait_recv)
    pl.when(greet_right)(to_left.wait_recv)
    aside = dot(jnp.where(has_left, left_v[...], zero), strips_v[0])
    aside += dot(jnp.where(has_right, right_v[...], zero), strips_v[1])
    spec_rows[:half] = (part[:half] + aside[:, : 2 * band]).astype(jnp.bfloat16)
    spec_rows[half:] = (part[half:] + aside[:, 2 * band :]).astype(jnp.bfloat16)
    pl.when(has_down)(to_down.start)
    pl.when(has_up)(to_up.start)
    mixed = dot(own_rows_v[...], spec_rows[...])
    pl.when(has_up)(to_down.wait_recv)
    pl.when(has_down)(to_up.wait_recv)
    zero = jnp.zeros((MARGIN, 2 * band), jnp.bfloat16)
    above = jnp.where(has_up, far_v[:MARGIN], zero)
    below = jnp.where(has_down, far_v[MARGIN:], zero)
    mixed += dot(far_rows_v[...], jnp.concatenate([above, below], axis=0))
    mixed *= 1.0 / ((core + 2 * MARGIN) * band)
    lower = lax.broadcasted_iota(jnp.int32, (band, 2 * band), 1) < band
    turned = pltpu.roll(mixed[band:], band, axis=1)
    spec = mixed[:band] + jnp.where(lower, turned, -turned)
    swapped = pltpu.roll(spec, band, axis=1)
    reals = jnp.where(lower, spec, swapped)
    imags = jnp.where(lower, swapped, -spec)

    steps = kerns // GROUP

    def first_half(s):
        c, g = divmod(s, steps)
        for i in range(GROUP // PACK):
            rows = []
            for j in range(PACK):
                held = kernels_v[c, g * GROUP + i * PACK + j].astype(jnp.float32)
                rows.append(
                    jnp.concatenate(
                        [(reals * held).astype(jnp.bfloat16), (imags * held).astype(jnp.bfloat16)],
                        axis=1,
                    )
                )
            out = nt_dot(first_v[...], jnp.concatenate(rows, axis=0)).astype(jnp.bfloat16)
            for j in range(PACK // 2):
                span = slice(j * 2 * band, (j + 1) * 2 * band)
                at = i * (PACK // 2) + j
                pair_v[s % 2, at * count : (at + 1) * count, : 2 * band] = out[:count, span]
                pair_v[s % 2, at * count : (at + 1) * count, 2 * band :] = out[count:, span]

    def second_half(s, level):
        c, g = divmod(s, steps)
        field = dot(pair_v[s % 2], second_v[...])
        for at in range(GROUP // 2):
            for i in range(2):
                re = field[at * count : (at + 1) * count, 2 * i * count : (2 * i + 1) * count]
                im = field[at * count : (at + 1) * count, (2 * i + 1) * count : (2 * i + 2) * count]
                term = weight_ref[c, g * GROUP + 2 * at + i] * (re * re + im * im)
                level = term if level is None else level + term
        return level

    rows_out = rows_out_v[cond]
    bounds = []

    def blur(level):
        fine, rest = halves(level)
        tall = nt_dot(rows_out, jnp.concatenate([fine, fine, rest], axis=1))
        fine, rest = halves(tall)
        logit = dot(jnp.concatenate([fine, fine, rest], axis=1), cols_out_v[...])
        if bounds:
            bounds[0] = jnp.maximum(bounds[0], logit)
            bounds[1] = jnp.minimum(bounds[1], logit)
        else:
            bounds.extend([logit, logit])

    level_copies = []
    first_half(0)
    level = None
    for s in range(conds * steps):
        c = s // steps
        if s + 1 < conds * steps:
            first_half(s + 1)
        level = second_half(s, level)
        if s % steps == steps - 1:
            total = weight_ref[c, 0]
            for k in range(1, kerns):
                total += weight_ref[c, k]
            scale = jnp.full((1, count), steepness * dose_ref[c]) / jnp.full((1, count), total)
            own_level[c] = level * scale - steepness * threshold_ref[c]
            copy = pltpu.make_async_remote_copy(
                src_ref=own_level.at[c],
                dst_ref=sib_level.at[c],
                send_sem=level_send.at[c],
                recv_sem=level_recv.at[c],
                device_id=sibling,
                device_id_type=MESH,
            )
            copy.start()
            level_copies.append(copy)
            level = None
            blur(own_level[c])
            if c > 0:
                level_copies[c - 1].wait_recv()
                blur(sib_level[c - 1])
    level_copies[-1].wait_recv()
    blur(sib_level[conds - 1])
    high_ref[0] = jax.nn.sigmoid(bounds[0])
    low_ref[0] = jax.nn.sigmoid(bounds[1])

    for flag, copy in (
        (greet_right, to_right),
        (greet_left, to_left),
        (has_down, to_down),
        (has_up, to_up),
    ):
        pl.when(flag)(copy.wait_send)
    for copy in level_copies:
        copy.wait_send()


def store_kernel(high_ref, low_ref, high_out, low_out, sem):
    copies = [
        pltpu.make_async_copy(high_ref, high_out, sem.at[0]),
        pltpu.make_async_copy(low_ref, low_out, sem.at[1]),
    ]
    for copy in copies:
        copy.start()
    for copy in copies:
        copy.wait()


def on_device(mask, kernels, socs_weight, dose, threshold):
    core = mask.shape[1]
    conds, kerns, band = kernels.shape[:3]
    tiles = lax.axis_size("tile")
    tables = [jnp.asarray(t) for t in make_tables(core, band)]
    count = (core + 2 * MARGIN) // STEP
    smem = pl.BlockSpec(memory_space=pltpu.SMEM)
    anywhere = pl.BlockSpec(memory_space=pl.ANY)
    vmem = pl.BlockSpec(memory_space=pltpu.VMEM)
    strip = (core // 2, LANES)
    seam = pl.pallas_call(
        functools.partial(seam_kernel, tiles),
        out_shape=jax.ShapeDtypeStruct(strip, mask.dtype),
        in_specs=[anywhere],
        out_specs=anywhere,
        scratch_shapes=[
            pltpu.VMEM(mask.shape[1:], mask.dtype),
            pltpu.VMEM(strip, mask.dtype),
            pltpu.SemaphoreType.DMA,
            pltpu.SemaphoreType.DMA,
            pltpu.SemaphoreType.DMA,
        ],
        compiler_params=pltpu.CompilerParams(collective_id=1, has_side_effects=True),
        name="seam",
    )(mask)
    loads = 2 + len(tables) + conds
    out = pltpu.VMEM((1, core // 2, core), jnp.float32)
    results = pl.pallas_call(
        functools.partial(kernel, tiles),
        out_shape=(out, out),
        in_specs=[anywhere, smem, smem] + [anywhere] * (3 + len(tables)),
        out_specs=(vmem, vmem),
        scratch_shapes=[
            pltpu.SMEM(socs_weight.shape, jnp.float32),
            pltpu.VMEM(mask.shape[1:], mask.dtype),
            pltpu.VMEM(kernels.shape, kernels.dtype),
            *[pltpu.VMEM(t.shape, t.dtype) for t in tables],
            pltpu.VMEM((2, *strip), mask.dtype),
            pltpu.VMEM(strip, mask.dtype),
            pltpu.VMEM(strip, mask.dtype),
            pltpu.VMEM((core, 2 * band), jnp.bfloat16),
            pltpu.VMEM((2 * MARGIN, 2 * band), jnp.bfloat16),
            pltpu.VMEM((2, GROUP // 2 * count, 4 * band), jnp.bfloat16),
            pltpu.VMEM((conds, count, count), jnp.float32),
            pltpu.VMEM((conds, count, count), jnp.float32),
            pltpu.SemaphoreType.DMA((loads,)),
            pltpu.SemaphoreType.DMA,
            pltpu.SemaphoreType.DMA((4,)),
            pltpu.SemaphoreType.DMA((4,)),
            pltpu.SemaphoreType.DMA((conds,)),
            pltpu.SemaphoreType.DMA((conds,)),
        ],
        compiler_params=pltpu.CompilerParams(collective_id=0, has_side_effects=True),
        name="expose",
    )(socs_weight, dose, threshold, mask, kernels, seam, *tables)
    final = jax.ShapeDtypeStruct((1, core // 2, core), jnp.float32)
    return pl.pallas_call(
        store_kernel,
        out_shape=(final, final),
        in_specs=[vmem, vmem],
        out_specs=(anywhere, anywhere),
        scratch_shapes=[pltpu.SemaphoreType.DMA((2,))],
        name="store",
    )(*(pltpu.with_memory_space_constraint(r, pltpu.VMEM) for r in results))


def solution(mesh):
    return jax.shard_map(
        on_device,
        mesh=mesh,
        in_specs=(
            P(("parts", "tile"), None, None),
            P("cond", None, None, None),
            P("cond", None),
            P("cond"),
            P("cond"),
        ),
        out_specs=(P(("parts", "tile"), "cond", None), P(("parts", "tile"), "cond", None)),
        check_vma=False,
    )
```

```python
import functools

import jax
import jax.numpy as jnp
import numpy as np
from jax import lax
from jax.experimental import pallas as pl
from jax.experimental.pallas import tpu as pltpu
from jax.sharding import PartitionSpec as P

MESH = pl.DeviceIdType.MESH
MARGIN = 64
BLUR = 8
LANES = 128
STEP = 3
PACK = 4
GROUP = 8

diffusion = 2.0
steepness = 8.0


def phase(pixels, pad_width, band_width):
    freq = np.arange(band_width) - band_width // 2
    angle = 2.0 * np.pi * ((pixels[:, None] * freq[None, :]) % pad_width) / pad_width
    return np.cos(angle), np.sin(angle)


def rounded_rows(exact):
    out = exact.astype(jnp.bfloat16).astype(np.float64)
    for row in out:
        for _ in range(64):
            excess = row.sum() - 1.0
            toward = np.full(row.shape, -np.inf if excess > 0 else np.inf).astype(jnp.bfloat16)
            moved = np.nextafter(row.astype(jnp.bfloat16), toward).astype(np.float64)
            left = np.abs(excess + moved - row)
            if excess == 0 or left.min() >= abs(excess):
                break
            row[left.argmin()] = moved[left.argmin()]
    return out


def make_tables(core, band_width):
    pad_width = core + 2 * MARGIN
    bf16 = lambda a: np.asarray(a, np.float32).astype(jnp.bfloat16)
    cos_in, sin_in = phase(np.arange(pad_width), pad_width, band_width)
    both = np.concatenate([cos_in, -sin_in], axis=1)
    columns = both[MARGIN : MARGIN + core]
    nil = np.zeros((MARGIN, 2 * band_width))
    strips = []
    for strip in (both[:MARGIN], both[MARGIN + core :]):
        strips.append(np.block([[strip, nil], [nil, strip]]))
    rows = np.concatenate([cos_in.T, sin_in.T], axis=0)
    own_rows = rows[:, MARGIN : MARGIN + core]
    far_rows = np.concatenate([rows[:, :MARGIN], rows[:, MARGIN + core :]], axis=1)
    count = pad_width // STEP
    cos_s, sin_s = phase(np.arange(count) * STEP, pad_width, band_width)
    first = np.block([[cos_s, -sin_s, -sin_s, cos_s], [sin_s, cos_s, cos_s, sin_s]])
    nil = np.zeros((band_width, count))
    second = np.block(
        [
            [cos_s.T, sin_s.T, nil, nil],
            [nil, nil, cos_s.T, sin_s.T],
            [-sin_s.T, cos_s.T, nil, nil],
            [nil, nil, -sin_s.T, cos_s.T],
        ]
    )
    offset = np.arange(core + 2 * BLUR)[None, :] - np.arange(core)[:, None] - BLUR
    taps = np.where(np.abs(offset) <= BLUR, np.exp(-(offset**2) / (2.0 * diffusion**2)), 0.0)
    reach = np.arange(-BLUR, BLUR + 1)
    taps = taps / np.sum(np.exp(-(reach**2) / (2.0 * diffusion**2)))
    pixel = np.arange(MARGIN - BLUR, MARGIN + core + BLUR)
    wave = np.arange(-(band_width - 1), band_width)
    apart = pixel[:, None] - STEP * np.arange(count)[None, :]
    interpolate = np.cos(2.0 * np.pi * apart[:, :, None] * wave / pad_width).sum(-1) / count
    smooth = taps @ interpolate
    smooth = rounded_rows(smooth)
    rows_out = np.concatenate([smooth, smooth], axis=1)
    cols_out = rows_out.T
    rows_out = rows_out.reshape(2, core // 2, 2 * count)
    return tuple(
        bf16(a) for a in (columns, np.stack(strips), own_rows, far_rows, first, second, rows_out, cols_out)
    )


def nt_dot(a, b):
    return lax.dot_general(a, b, (((1,), (1,)), ((), ())), preferred_element_type=jnp.float32)


def dot(a, b):
    return jnp.dot(a, b, preferred_element_type=jnp.float32)


def halves(a):
    high = a.astype(jnp.bfloat16)
    return high, (a - high.astype(jnp.float32)).astype(jnp.bfloat16)


def spot(tiles):
    grid_cols = min(8, tiles // 2)
    place = lax.rem(lax.axis_index("tile") + grid_cols // 2, tiles)
    column = lax.rem(place, grid_cols)
    row = lax.div(place, grid_cols)
    odd = lax.rem(row, 2) == 1
    seam_left = jnp.logical_and(odd, column == grid_cols // 2)
    seam_right = jnp.logical_and(odd, column == grid_cols // 2 - 1)
    return grid_cols, column, row, seam_left, seam_right


def last_columns(mask_v):
    rows, columns = mask_v.shape
    upper = mask_v[: rows // 2, columns - LANES :].astype(jnp.float32)
    lower = mask_v[rows // 2 :, columns - LANES :].astype(jnp.float32)
    early = lax.broadcasted_iota(jnp.int32, upper.shape, 1) < MARGIN
    return jnp.where(early, pltpu.roll(upper, MARGIN, axis=1), lower).astype(mask_v.dtype)


def first_columns(mask_v):
    rows = mask_v.shape[0]
    upper = mask_v[: rows // 2, :LANES].astype(jnp.float32)
    lower = mask_v[rows // 2 :, :LANES].astype(jnp.float32)
    early = lax.broadcasted_iota(jnp.int32, upper.shape, 1) < MARGIN
    return jnp.where(early, upper, pltpu.roll(lower, MARGIN, axis=1)).astype(mask_v.dtype)


def seam_kernel(tiles, mask_hbm, strip_hbm, mask_v, packed_v, load_sem, send_sem, recv_sem):
    tile = lax.axis_index("tile")
    _, _, _, seam_left, seam_right = spot(tiles)

    def exchange(peer, pack):
        barrier = pltpu.get_barrier_semaphore()
        pl.semaphore_signal(barrier, inc=1, device_id=peer, device_id_type=MESH)
        load = pltpu.make_async_copy(mask_hbm.at[0], mask_v, load_sem)
        load.start()
        load.wait()
        packed_v[...] = pack(mask_v)
        pl.semaphore_wait(barrier, 1)
        copy = pltpu.make_async_remote_copy(
            src_ref=packed_v,
            dst_ref=strip_hbm,
            send_sem=send_sem,
            recv_sem=recv_sem,
            device_id=peer,
            device_id_type=MESH,
        )
        copy.start()
        copy.wait()

    @pl.when(seam_right)
    def _():
        exchange({"tile": lax.rem(tile + 1, tiles)}, last_columns)

    @pl.when(seam_left)
    def _():
        exchange({"tile": lax.rem(tile + tiles - 1, tiles)}, first_columns)


def kernel(
    tiles,
    weight_hbm,
    dose_hbm,
    threshold_hbm,
    mask_hbm,
    kernels_hbm,
    strip_hbm,
    columns_hbm,
    strips_hbm,
    own_rows_hbm,
    far_rows_hbm,
    first_hbm,
    second_hbm,
    rows_out_hbm,
    cols_out_hbm,
    high_ref,
    low_ref,
    weight_ref,
    dose_ref,
    threshold_ref,
    mask_v,
    kernels_v,
    columns_v,
    strips_v,
    own_rows_v,
    far_rows_v,
    first_v,
    second_v,
    rows_out_v,
    cols_out_v,
    packed_v,
    left_v,
    right_v,
    spec_rows,
    far_v,
    pair_v,
    own_level,
    sib_level,
    load_sem,
    strip_sem,
    send_sem,
    recv_sem,
    level_send,
    level_recv,
):
    conds, kerns, band = kernels_v.shape[:3]
    core = mask_v.shape[0]
    half = core // 2
    count = own_level.shape[1]
    tile = lax.axis_index("tile")
    cond = lax.axis_index("cond")
    grid_cols, column, row, seam_left, seam_right = spot(tiles)
    has_left = column > 0
    has_right = column < grid_cols - 1
    has_up = row > 0
    has_down = row < tiles // grid_cols - 1
    greet_left = jnp.logical_and(has_left, jnp.logical_not(seam_left))
    greet_right = jnp.logical_and(has_right, jnp.logical_not(seam_right))
    right = {"tile": lax.rem(tile + 1, tiles)}
    left = {"tile": lax.rem(tile + tiles - 1, tiles)}
    far = {"tile": lax.rem(tile + tiles + grid_cols * (2 * cond - 1), tiles), "cond": 1 - cond}
    far_row = row + 2 * cond - 1
    has_far = jnp.logical_and(far_row >= 0, far_row < tiles // grid_cols)
    other_row = row + 1 - 2 * cond
    has_other = jnp.logical_and(other_row >= 0, other_row < tiles // grid_cols)
    sibling = {"cond": 1 - cond}

    sources = (
        mask_hbm.at[0],
        columns_hbm,
        strips_hbm,
        own_rows_hbm,
        far_rows_hbm,
        first_hbm,
        second_hbm,
        weight_hbm,
        dose_hbm,
        threshold_hbm,
        rows_out_hbm,
        cols_out_hbm,
        *[kernels_hbm.at[c] for c in range(conds)],
    )
    targets = (
        mask_v,
        columns_v,
        strips_v,
        own_rows_v,
        far_rows_v,
        first_v,
        second_v,
        weight_ref,
        dose_ref,
        threshold_ref,
        rows_out_v,
        cols_out_v,
        *[kernels_v.at[c] for c in range(conds)],
    )
    loads = [
        pltpu.make_async_copy(s, t, load_sem.at[i]) for i, (s, t) in enumerate(zip(sources, targets))
    ]
    loads[0].start()
    barrier = pltpu.get_barrier_semaphore()
    peers = 1
    for flag, peer in ((has_far, far), (greet_left, left), (greet_right, right)):
        peers = peers + flag.astype(jnp.int32)

        @pl.when(flag)
        def _(peer=peer):
            pl.semaphore_signal(barrier, inc=1, device_id=peer, device_id_type=MESH)

    pl.semaphore_signal(barrier, inc=1, device_id=sibling, device_id_type=MESH)
    for load in loads[1:]:
        load.start()
    from_seam = [
        (seam_left, pltpu.make_async_copy(strip_hbm, left_v, strip_sem)),
        (seam_right, pltpu.make_async_copy(strip_hbm, right_v, strip_sem)),
    ]
    for flag, copy in from_seam:
        pl.when(flag)(copy.start)

    def remote(src, dst, i, peer):
        return pltpu.make_async_remote_copy(
            src_ref=src,
            dst_ref=dst,
            send_sem=send_sem.at[i],
            recv_sem=recv_sem.at[i],
            device_id=peer,
            device_id_type=MESH,
        )

    to_right = remote(packed_v.at[0], left_v, 0, right)
    to_left = remote(packed_v.at[1], right_v, 1, left)
    edge = pl.ds(pl.multiple_of(cond * (core - MARGIN), MARGIN), MARGIN)
    to_far = remote(spec_rows.at[edge], far_v.at[1 - cond], 2, far)
    to_sibling = remote(far_v.at[cond], far_v.at[cond], 3, sibling)
    from_sibling = remote(far_v.at[1 - cond], far_v.at[1 - cond], 3, sibling)

    loads[0].wait()
    packed_v[0] = last_columns(mask_v)
    packed_v[1] = first_columns(mask_v)
    pl.semaphore_wait(barrier, peers)
    pl.when(greet_right)(to_right.start)
    pl.when(greet_left)(to_left.start)

    for load in loads[1:]:
        load.wait()
    part = dot(mask_v[...], columns_v[...])
    zero = jnp.zeros((half, LANES), jnp.bfloat16)
    pl.when(seam_left)(from_seam[0][1].wait)
    pl.when(seam_right)(from_seam[1][1].wait)
    pl.when(greet_left)(to_right.wait_recv)
    pl.when(greet_right)(to_left.wait_recv)
    aside = dot(jnp.where(has_left, left_v[...], zero), strips_v[0])
    aside += dot(jnp.where(has_right, right_v[...], zero), strips_v[1])
    spec_rows[:half] = (part[:half] + aside[:, : 2 * band]).astype(jnp.bfloat16)
    spec_rows[half:] = (part[half:] + aside[:, 2 * band :]).astype(jnp.bfloat16)
    pl.when(has_far)(to_far.start)
    mixed = dot(own_rows_v[...], spec_rows[...])

    @pl.when(has_far)
    def _():
        to_far.wait_recv()
        to_sibling.start()

    pl.when(has_other)(from_sibling.wait_recv)
    zero = jnp.zeros((MARGIN, 2 * band), jnp.bfloat16)
    above = jnp.where(has_up, far_v[0], zero)
    below = jnp.where(has_down, far_v[1], zero)
    mixed += dot(far_rows_v[...], jnp.concatenate([above, below], axis=0))
    mixed *= 1.0 / ((core + 2 * MARGIN) * band)
    lower = lax.broadcasted_iota(jnp.int32, (band, 2 * band), 1) < band
    turned = pltpu.roll(mixed[band:], band, axis=1)
    spec = mixed[:band] + jnp.where(lower, turned, -turned)
    swapped = pltpu.roll(spec, band, axis=1)
    reals = jnp.where(lower, spec, swapped)
    imags = jnp.where(lower, swapped, -spec)

    steps = kerns // GROUP

    def first_half(s):
        c, g = divmod(s, steps)
        for i in range(GROUP // PACK):
            rows = []
            for j in range(PACK):
                held = kernels_v[c, g * GROUP + i * PACK + j].astype(jnp.float32)
                rows.append(
                    jnp.concatenate(
                        [(reals * held).astype(jnp.bfloat16), (imags * held).astype(jnp.bfloat16)],
                        axis=1,
                    )
                )
            out = nt_dot(first_v[...], jnp.concatenate(rows, axis=0)).astype(jnp.bfloat16)
            for j in range(PACK // 2):
                span = slice(j * 2 * band, (j + 1) * 2 * band)
                at = i * (PACK // 2) + j
                pair_v[s % 2, at * count : (at + 1) * count, : 2 * band] = out[:count, span]
                pair_v[s % 2, at * count : (at + 1) * count, 2 * band :] = out[count:, span]

    def second_half(s, level):
        c, g = divmod(s, steps)
        field = dot(pair_v[s % 2], second_v[...])
        for at in range(GROUP // 2):
            for i in range(2):
                re = field[at * count : (at + 1) * count, 2 * i * count : (2 * i + 1) * count]
                im = field[at * count : (at + 1) * count, (2 * i + 1) * count : (2 * i + 2) * count]
                term = weight_ref[c, g * GROUP + 2 * at + i] * (re * re + im * im)
                level = term if level is None else level + term
        return level

    rows_out = rows_out_v[cond]
    bounds = []

    def blur(level):
        fine, rest = halves(level)
        tall = nt_dot(rows_out, jnp.concatenate([fine, rest], axis=1))
        fine, rest = halves(tall)
        logit = dot(jnp.concatenate([fine, rest], axis=1), cols_out_v[...])
        if bounds:
            bounds[0] = jnp.maximum(bounds[0], logit)
            bounds[1] = jnp.minimum(bounds[1], logit)
        else:
            bounds.extend([logit, logit])

    level_copies = []
    ready = []
    first_half(0)
    level = None
    for s in range(conds * steps):
        c = s // steps
        if s + 1 < conds * steps:
            first_half(s + 1)
        level = second_half(s, level)
        if s % steps == steps - 1:
            for ref in ready:
                blur(ref[...])
            ready = [own_level.at[c]]
            total = weight_ref[c, 0]
            for k in range(1, kerns):
                total += weight_ref[c, k]
            scale = jnp.full((1, count), steepness * dose_ref[c]) / jnp.full((1, count), total)
            own_level[c] = level * scale - steepness * threshold_ref[c]
            copy = pltpu.make_async_remote_copy(
                src_ref=own_level.at[c],
                dst_ref=sib_level.at[c],
                send_sem=level_send.at[c],
                recv_sem=level_recv.at[c],
                device_id=sibling,
                device_id_type=MESH,
            )
            copy.start()
            level_copies.append(copy)
            level = None
            if c > 0:
                level_copies[c - 1].wait_recv()
                ready.append(sib_level.at[c - 1])
    for ref in ready:
        blur(ref[...])
    level_copies[-1].wait_recv()
    blur(sib_level[conds - 1])
    high_ref[0] = jax.nn.sigmoid(bounds[0])
    low_ref[0] = jax.nn.sigmoid(bounds[1])

    for flag, copy in (
        (greet_right, to_right),
        (greet_left, to_left),
        (has_far, to_far),
        (has_far, to_sibling),
    ):
        pl.when(flag)(copy.wait_send)
    for copy in level_copies:
        copy.wait_send()


def store_kernel(high_ref, low_ref, high_out, low_out, sem):
    copies = [
        pltpu.make_async_copy(high_ref, high_out, sem.at[0]),
        pltpu.make_async_copy(low_ref, low_out, sem.at[1]),
    ]
    for copy in copies:
        copy.start()
    for copy in copies:
        copy.wait()


def on_device(mask, kernels, socs_weight, dose, threshold):
    core = mask.shape[1]
    conds, kerns, band = kernels.shape[:3]
    tiles = lax.axis_size("tile")
    tables = [jnp.asarray(t) for t in make_tables(core, band)]
    count = (core + 2 * MARGIN) // STEP
    anywhere = pl.BlockSpec(memory_space=pl.ANY)
    vmem = pl.BlockSpec(memory_space=pltpu.VMEM)
    strip = (core // 2, LANES)
    seam = pl.pallas_call(
        functools.partial(seam_kernel, tiles),
        out_shape=jax.ShapeDtypeStruct(strip, mask.dtype),
        in_specs=[anywhere],
        out_specs=anywhere,
        scratch_shapes=[
            pltpu.VMEM(mask.shape[1:], mask.dtype),
            pltpu.VMEM(strip, mask.dtype),
            pltpu.SemaphoreType.DMA,
            pltpu.SemaphoreType.DMA,
            pltpu.SemaphoreType.DMA,
        ],
        compiler_params=pltpu.CompilerParams(collective_id=1, has_side_effects=True),
        name="seam",
    )(mask)
    loads = 4 + len(tables) + conds
    out = pltpu.VMEM((1, core // 2, core), jnp.float32)
    results = pl.pallas_call(
        functools.partial(kernel, tiles),
        out_shape=(out, out),
        in_specs=[anywhere] * (6 + len(tables)),
        out_specs=(vmem, vmem),
        scratch_shapes=[
            *[pltpu.SMEM(a.shape, a.dtype) for a in (socs_weight, dose, threshold)],
            pltpu.VMEM(mask.shape[1:], mask.dtype),
            pltpu.VMEM(kernels.shape, kernels.dtype),
            *[pltpu.VMEM(t.shape, t.dtype) for t in tables],
            pltpu.VMEM((2, *strip), mask.dtype),
            pltpu.VMEM(strip, mask.dtype),
            pltpu.VMEM(strip, mask.dtype),
            pltpu.VMEM((core, 2 * band), jnp.bfloat16),
            pltpu.VMEM((2, MARGIN, 2 * band), jnp.bfloat16),
            pltpu.VMEM((2, GROUP // 2 * count, 4 * band), jnp.bfloat16),
            pltpu.VMEM((conds, count, count), jnp.float32),
            pltpu.VMEM((conds, count, count), jnp.float32),
            pltpu.SemaphoreType.DMA((loads,)),
            pltpu.SemaphoreType.DMA,
            pltpu.SemaphoreType.DMA((4,)),
            pltpu.SemaphoreType.DMA((4,)),
            pltpu.SemaphoreType.DMA((conds,)),
            pltpu.SemaphoreType.DMA((conds,)),
        ],
        compiler_params=pltpu.CompilerParams(collective_id=0, has_side_effects=True),
        name="expose",
    )(socs_weight, dose, threshold, mask, kernels, seam, *tables)
    final = jax.ShapeDtypeStruct((1, core // 2, core), jnp.float32)
    return pl.pallas_call(
        store_kernel,
        out_shape=(final, final),
        in_specs=[vmem, vmem],
        out_specs=(anywhere, anywhere),
        scratch_shapes=[pltpu.SemaphoreType.DMA((2,))],
        name="store",
    )(*(pltpu.with_memory_space_constraint(r, pltpu.VMEM) for r in results))


def solution(mesh):
    return jax.shard_map(
        on_device,
        mesh=mesh,
        in_specs=(
            P(("parts", "tile"), None, None),
            P("cond", None, None, None),
            P("cond", None),
            P("cond"),
            P("cond"),
        ),
        out_specs=(P(("parts", "tile"), "cond", None), P(("parts", "tile"), "cond", None)),
        check_vma=False,
    )
```

```python
import functools

import jax
import jax.numpy as jnp
import numpy as np
from jax import lax
from jax.experimental import pallas as pl
from jax.experimental.pallas import tpu as pltpu
from jax.sharding import PartitionSpec as P

MESH = pl.DeviceIdType.MESH
MARGIN = 64
BLUR = 8
LANES = 128
STEP = 3
PACK = 4
GROUP = 8

diffusion = 2.0
steepness = 8.0


def phase(pixels, pad_width, band_width):
    freq = np.arange(band_width) - band_width // 2
    angle = 2.0 * np.pi * ((pixels[:, None] * freq[None, :]) % pad_width) / pad_width
    return np.cos(angle), np.sin(angle)


def rounded_rows(exact):
    out = exact.astype(jnp.bfloat16).astype(np.float64)
    for row in out:
        for _ in range(64):
            excess = row.sum() - 1.0
            toward = np.full(row.shape, -np.inf if excess > 0 else np.inf).astype(jnp.bfloat16)
            moved = np.nextafter(row.astype(jnp.bfloat16), toward).astype(np.float64)
            left = np.abs(excess + moved - row)
            if excess == 0 or left.min() >= abs(excess):
                break
            row[left.argmin()] = moved[left.argmin()]
    return out


def make_tables(core, band_width):
    pad_width = core + 2 * MARGIN
    bf16 = lambda a: np.asarray(a, np.float32).astype(jnp.bfloat16)
    cos_in, sin_in = phase(np.arange(pad_width), pad_width, band_width)
    both = np.concatenate([cos_in, -sin_in], axis=1)
    columns = both[MARGIN : MARGIN + core]
    nil = np.zeros((MARGIN, 2 * band_width))
    strips = []
    for strip in (both[:MARGIN], both[MARGIN + core :]):
        strips.append(np.block([[strip, nil], [nil, strip]]))
    rows = np.concatenate([cos_in.T, sin_in.T], axis=0)
    own_rows = rows[:, MARGIN : MARGIN + core]
    far_rows = np.concatenate([rows[:, :MARGIN], rows[:, MARGIN + core :]], axis=1)
    count = pad_width // STEP
    cos_s, sin_s = phase(np.arange(count) * STEP, pad_width, band_width)
    first = np.block([[cos_s, -sin_s, -sin_s, cos_s], [sin_s, cos_s, cos_s, sin_s]])
    nil = np.zeros((band_width, count))
    second = np.block(
        [
            [cos_s.T, sin_s.T, nil, nil],
            [nil, nil, cos_s.T, sin_s.T],
            [-sin_s.T, cos_s.T, nil, nil],
            [nil, nil, -sin_s.T, cos_s.T],
        ]
    )
    offset = np.arange(core + 2 * BLUR)[None, :] - np.arange(core)[:, None] - BLUR
    taps = np.where(np.abs(offset) <= BLUR, np.exp(-(offset**2) / (2.0 * diffusion**2)), 0.0)
    reach = np.arange(-BLUR, BLUR + 1)
    taps = taps / np.sum(np.exp(-(reach**2) / (2.0 * diffusion**2)))
    pixel = np.arange(MARGIN - BLUR, MARGIN + core + BLUR)
    wave = np.arange(-(band_width - 1), band_width)
    apart = pixel[:, None] - STEP * np.arange(count)[None, :]
    interpolate = np.cos(2.0 * np.pi * apart[:, :, None] * wave / pad_width).sum(-1) / count
    smooth = taps @ interpolate
    smooth = rounded_rows(smooth)
    rows_out = np.concatenate([smooth, smooth], axis=1)
    cols_out = rows_out.T
    rows_out = rows_out.reshape(2, core // 2, 2 * count)
    return tuple(
        bf16(a) for a in (columns, np.stack(strips), own_rows, far_rows, first, second, rows_out, cols_out)
    )


def nt_dot(a, b):
    return lax.dot_general(a, b, (((1,), (1,)), ((), ())), preferred_element_type=jnp.float32)


def dot(a, b):
    return jnp.dot(a, b, preferred_element_type=jnp.float32)


def halves(a):
    high = a.astype(jnp.bfloat16)
    return high, (a - high.astype(jnp.float32)).astype(jnp.bfloat16)


def spot(tiles):
    grid_cols = min(8, tiles // 2)
    place = lax.rem(lax.axis_index("tile") + grid_cols // 2, tiles)
    column = lax.rem(place, grid_cols)
    row = lax.div(place, grid_cols)
    odd = lax.rem(row, 2) == 1
    seam_left = jnp.logical_and(odd, column == grid_cols // 2)
    seam_right = jnp.logical_and(odd, column == grid_cols // 2 - 1)
    return grid_cols, column, row, seam_left, seam_right


def last_columns(mask_v):
    rows, columns = mask_v.shape
    upper = mask_v[: rows // 2, columns - LANES :].astype(jnp.float32)
    lower = mask_v[rows // 2 :, columns - LANES :].astype(jnp.float32)
    early = lax.broadcasted_iota(jnp.int32, upper.shape, 1) < MARGIN
    return jnp.where(early, pltpu.roll(upper, MARGIN, axis=1), lower).astype(mask_v.dtype)


def first_columns(mask_v):
    rows = mask_v.shape[0]
    upper = mask_v[: rows // 2, :LANES].astype(jnp.float32)
    lower = mask_v[rows // 2 :, :LANES].astype(jnp.float32)
    early = lax.broadcasted_iota(jnp.int32, upper.shape, 1) < MARGIN
    return jnp.where(early, upper, pltpu.roll(lower, MARGIN, axis=1)).astype(mask_v.dtype)


def seam_kernel(tiles, mask_hbm, strip_hbm, mask_v, packed_v, load_sem, send_sem, recv_sem):
    tile = lax.axis_index("tile")
    _, _, _, seam_left, seam_right = spot(tiles)

    def exchange(peer, pack):
        barrier = pltpu.get_barrier_semaphore()
        pl.semaphore_signal(barrier, inc=1, device_id=peer, device_id_type=MESH)
        load = pltpu.make_async_copy(mask_hbm.at[0], mask_v, load_sem)
        load.start()
        load.wait()
        packed_v[...] = pack(mask_v)
        pl.semaphore_wait(barrier, 1)
        copy = pltpu.make_async_remote_copy(
            src_ref=packed_v,
            dst_ref=strip_hbm,
            send_sem=send_sem,
            recv_sem=recv_sem,
            device_id=peer,
            device_id_type=MESH,
        )
        copy.start()
        copy.wait()

    @pl.when(seam_right)
    def _():
        exchange({"tile": lax.rem(tile + 1, tiles)}, last_columns)

    @pl.when(seam_left)
    def _():
        exchange({"tile": lax.rem(tile + tiles - 1, tiles)}, first_columns)


def kernel(
    tiles,
    weight_hbm,
    dose_hbm,
    threshold_hbm,
    mask_ref,
    kernels_hbm,
    strip_hbm,
    columns_hbm,
    strips_hbm,
    own_rows_hbm,
    far_rows_hbm,
    first_hbm,
    second_hbm,
    rows_out_hbm,
    cols_out_hbm,
    high_ref,
    low_ref,
    weight_ref,
    dose_ref,
    threshold_ref,
    kernels_v,
    columns_v,
    strips_v,
    own_rows_v,
    far_rows_v,
    first_v,
    second_v,
    rows_out_v,
    cols_out_v,
    packed_v,
    left_v,
    right_v,
    spec_rows,
    far_v,
    pair_v,
    own_level,
    sib_level,
    load_sem,
    strip_sem,
    send_sem,
    recv_sem,
    level_send,
    level_recv,
):
    conds, kerns, band = kernels_v.shape[:3]
    mask_v = mask_ref.at[0]
    core = mask_v.shape[0]
    half = core // 2
    count = own_level.shape[1]
    tile = lax.axis_index("tile")
    cond = lax.axis_index("cond")
    grid_cols, column, row, seam_left, seam_right = spot(tiles)
    has_left = column > 0
    has_right = column < grid_cols - 1
    has_up = row > 0
    has_down = row < tiles // grid_cols - 1
    greet_left = jnp.logical_and(has_left, jnp.logical_not(seam_left))
    greet_right = jnp.logical_and(has_right, jnp.logical_not(seam_right))
    right = {"tile": lax.rem(tile + 1, tiles)}
    left = {"tile": lax.rem(tile + tiles - 1, tiles)}
    far = {"tile": lax.rem(tile + tiles + grid_cols * (2 * cond - 1), tiles), "cond": 1 - cond}
    far_row = row + 2 * cond - 1
    has_far = jnp.logical_and(far_row >= 0, far_row < tiles // grid_cols)
    other_row = row + 1 - 2 * cond
    has_other = jnp.logical_and(other_row >= 0, other_row < tiles // grid_cols)
    sibling = {"cond": 1 - cond}

    sources = (
        columns_hbm,
        strips_hbm,
        own_rows_hbm,
        far_rows_hbm,
        first_hbm,
        second_hbm,
        weight_hbm,
        dose_hbm,
        threshold_hbm,
        rows_out_hbm,
        cols_out_hbm,
        *[kernels_hbm.at[c] for c in range(conds)],
    )
    targets = (
        columns_v,
        strips_v,
        own_rows_v,
        far_rows_v,
        first_v,
        second_v,
        weight_ref,
        dose_ref,
        threshold_ref,
        rows_out_v,
        cols_out_v,
        *[kernels_v.at[c] for c in range(conds)],
    )
    loads = [
        pltpu.make_async_copy(s, t, load_sem.at[i]) for i, (s, t) in enumerate(zip(sources, targets))
    ]
    barrier = pltpu.get_barrier_semaphore()
    peers = 1
    for flag, peer in ((has_far, far), (greet_left, left), (greet_right, right)):
        peers = peers + flag.astype(jnp.int32)

        @pl.when(flag)
        def _(peer=peer):
            pl.semaphore_signal(barrier, inc=1, device_id=peer, device_id_type=MESH)

    pl.semaphore_signal(barrier, inc=1, device_id=sibling, device_id_type=MESH)
    from_seam = [
        (seam_left, pltpu.make_async_copy(strip_hbm, left_v, strip_sem)),
        (seam_right, pltpu.make_async_copy(strip_hbm, right_v, strip_sem)),
    ]
    for flag, copy in from_seam:
        pl.when(flag)(copy.start)

    def remote(src, dst, i, peer):
        return pltpu.make_async_remote_copy(
            src_ref=src,
            dst_ref=dst,
            send_sem=send_sem.at[i],
            recv_sem=recv_sem.at[i],
            device_id=peer,
            device_id_type=MESH,
        )

    to_right = remote(packed_v.at[0], left_v, 0, right)
    to_left = remote(packed_v.at[1], right_v, 1, left)
    edge = pl.ds(pl.multiple_of(cond * (core - MARGIN), MARGIN), MARGIN)
    to_far = remote(spec_rows.at[edge], far_v.at[1 - cond], 2, far)
    to_sibling = remote(far_v.at[cond], far_v.at[cond], 3, sibling)
    from_sibling = remote(far_v.at[1 - cond], far_v.at[1 - cond], 3, sibling)

    packed_v[0] = last_columns(mask_v)
    packed_v[1] = first_columns(mask_v)
    pl.semaphore_wait(barrier, peers)
    pl.when(greet_right)(to_right.start)
    pl.when(greet_left)(to_left.start)
    for load in loads:
        load.start()

    for load in loads:
        load.wait()
    part = dot(mask_v[...], columns_v[...])
    zero = jnp.zeros((half, LANES), jnp.bfloat16)
    pl.when(seam_left)(from_seam[0][1].wait)
    pl.when(seam_right)(from_seam[1][1].wait)
    pl.when(greet_left)(to_right.wait_recv)
    pl.when(greet_right)(to_left.wait_recv)
    aside = dot(jnp.where(has_left, left_v[...], zero), strips_v[0])
    aside += dot(jnp.where(has_right, right_v[...], zero), strips_v[1])
    spec_rows[:half] = (part[:half] + aside[:, : 2 * band]).astype(jnp.bfloat16)
    spec_rows[half:] = (part[half:] + aside[:, 2 * band :]).astype(jnp.bfloat16)
    pl.when(has_far)(to_far.start)
    mixed = dot(own_rows_v[...], spec_rows[...])

    @pl.when(has_far)
    def _():
        to_far.wait_recv()
        to_sibling.start()

    pl.when(has_other)(from_sibling.wait_recv)
    zero = jnp.zeros((MARGIN, 2 * band), jnp.bfloat16)
    above = jnp.where(has_up, far_v[0], zero)
    below = jnp.where(has_down, far_v[1], zero)
    mixed += dot(far_rows_v[...], jnp.concatenate([above, below], axis=0))
    mixed *= 1.0 / ((core + 2 * MARGIN) * band)
    lower = lax.broadcasted_iota(jnp.int32, (band, 2 * band), 1) < band
    turned = pltpu.roll(mixed[band:], band, axis=1)
    spec = mixed[:band] + jnp.where(lower, turned, -turned)
    swapped = pltpu.roll(spec, band, axis=1)
    reals = jnp.where(lower, spec, swapped)
    imags = jnp.where(lower, swapped, -spec)

    steps = kerns // GROUP

    def first_half(s):
        c, g = divmod(s, steps)
        for i in range(GROUP // PACK):
            rows = []
            for j in range(PACK):
                held = kernels_v[c, g * GROUP + i * PACK + j].astype(jnp.float32)
                rows.append(
                    jnp.concatenate(
                        [(reals * held).astype(jnp.bfloat16), (imags * held).astype(jnp.bfloat16)],
                        axis=1,
                    )
                )
            out = nt_dot(first_v[...], jnp.concatenate(rows, axis=0)).astype(jnp.bfloat16)
            for j in range(PACK // 2):
                span = slice(j * 2 * band, (j + 1) * 2 * band)
                at = i * (PACK // 2) + j
                pair_v[s % 2, at * count : (at + 1) * count, : 2 * band] = out[:count, span]
                pair_v[s % 2, at * count : (at + 1) * count, 2 * band :] = out[count:, span]

    def second_half(s, level):
        c, g = divmod(s, steps)
        field = dot(pair_v[s % 2], second_v[...])
        for at in range(GROUP // 2):
            for i in range(2):
                re = field[at * count : (at + 1) * count, 2 * i * count : (2 * i + 1) * count]
                im = field[at * count : (at + 1) * count, (2 * i + 1) * count : (2 * i + 2) * count]
                term = weight_ref[c, g * GROUP + 2 * at + i] * (re * re + im * im)
                level = term if level is None else level + term
        return level

    rows_out = rows_out_v[cond]
    bounds = []

    def blur(levels):
        talls = []
        for level in levels:
            fine, rest = halves(level[...])
            tall = nt_dot(rows_out, jnp.concatenate([fine, rest], axis=1))
            talls.append(jnp.concatenate(halves(tall), axis=1))
        logits = dot(jnp.concatenate(talls, axis=0), cols_out_v[...])
        for i in range(len(levels)):
            logit = logits[i * half : (i + 1) * half]
            if bounds:
                bounds[0] = jnp.maximum(bounds[0], logit)
                bounds[1] = jnp.minimum(bounds[1], logit)
            else:
                bounds.extend([logit, logit])

    def finish(c, level):
        total = weight_ref[c, 0]
        for k in range(1, kerns):
            total += weight_ref[c, k]
        scale = jnp.full((1, count), steepness * dose_ref[c]) / jnp.full((1, count), total)
        own_level[c] = level * scale - steepness * threshold_ref[c]
        copy = pltpu.make_async_remote_copy(
            src_ref=own_level.at[c],
            dst_ref=sib_level.at[c],
            send_sem=level_send.at[c],
            recv_sem=level_recv.at[c],
            device_id=sibling,
            device_id_type=MESH,
        )
        copy.start()
        level_copies.append(copy)

    level_copies = []
    level = None
    levels = []
    first_half(0)
    for s in range(conds * steps):
        c = s // steps
        if s + 1 < conds * steps:
            first_half(s + 1)
        level = second_half(s, level)
        if s % steps == steps - 1:
            levels.append(level)
            level = None
            if c == conds - 2:
                for i in range(conds - 1):
                    finish(i, levels[i])
    finish(conds - 1, levels[-1])
    blur([own_level.at[c] for c in range(conds)])
    for copy in level_copies[:-1]:
        copy.wait_recv()
    blur([sib_level.at[c] for c in range(conds - 1)])
    level_copies[-1].wait_recv()
    blur([sib_level.at[conds - 1]])
    high_ref[0] = jax.nn.sigmoid(bounds[0])
    low_ref[0] = jax.nn.sigmoid(bounds[1])

    for flag, copy in (
        (greet_right, to_right),
        (greet_left, to_left),
        (has_far, to_far),
        (has_far, to_sibling),
    ):
        pl.when(flag)(copy.wait_send)
    for copy in level_copies:
        copy.wait_send()


def store_kernel(high_ref, low_ref, high_out, low_out, sem):
    copies = [
        pltpu.make_async_copy(high_ref, high_out, sem.at[0]),
        pltpu.make_async_copy(low_ref, low_out, sem.at[1]),
    ]
    for copy in copies:
        copy.start()
    for copy in copies:
        copy.wait()


def on_device(mask, kernels, socs_weight, dose, threshold):
    core = mask.shape[1]
    conds, kerns, band = kernels.shape[:3]
    tiles = lax.axis_size("tile")
    tables = [jnp.asarray(t) for t in make_tables(core, band)]
    count = (core + 2 * MARGIN) // STEP
    anywhere = pl.BlockSpec(memory_space=pl.ANY)
    vmem = pl.BlockSpec(memory_space=pltpu.VMEM)
    strip = (core // 2, LANES)
    seam = pl.pallas_call(
        functools.partial(seam_kernel, tiles),
        out_shape=jax.ShapeDtypeStruct(strip, mask.dtype),
        in_specs=[anywhere],
        out_specs=anywhere,
        scratch_shapes=[
            pltpu.VMEM(mask.shape[1:], mask.dtype),
            pltpu.VMEM(strip, mask.dtype),
            pltpu.SemaphoreType.DMA,
            pltpu.SemaphoreType.DMA,
            pltpu.SemaphoreType.DMA,
        ],
        compiler_params=pltpu.CompilerParams(collective_id=1, has_side_effects=True),
        cost_estimate=pl.CostEstimate(flops=10**9, bytes_accessed=4 * mask.size, transcendentals=0),
        name="seam",
    )(mask)
    loads = 3 + len(tables) + conds
    out = pltpu.VMEM((1, core // 2, core), jnp.float32)
    results = pl.pallas_call(
        functools.partial(kernel, tiles),
        out_shape=(out, out),
        in_specs=[anywhere] * 3 + [vmem] + [anywhere] * (2 + len(tables)),
        out_specs=(vmem, vmem),
        scratch_shapes=[
            *[pltpu.SMEM(a.shape, a.dtype) for a in (socs_weight, dose, threshold)],
            pltpu.VMEM(kernels.shape, kernels.dtype),
            *[pltpu.VMEM(t.shape, t.dtype) for t in tables],
            pltpu.VMEM((2, *strip), mask.dtype),
            pltpu.VMEM(strip, mask.dtype),
            pltpu.VMEM(strip, mask.dtype),
            pltpu.VMEM((core, 2 * band), jnp.bfloat16),
            pltpu.VMEM((2, MARGIN, 2 * band), jnp.bfloat16),
            pltpu.VMEM((2, GROUP // 2 * count, 4 * band), jnp.bfloat16),
            pltpu.VMEM((conds, count, count), jnp.float32),
            pltpu.VMEM((conds, count, count), jnp.float32),
            pltpu.SemaphoreType.DMA((loads,)),
            pltpu.SemaphoreType.DMA,
            pltpu.SemaphoreType.DMA((4,)),
            pltpu.SemaphoreType.DMA((4,)),
            pltpu.SemaphoreType.DMA((conds,)),
            pltpu.SemaphoreType.DMA((conds,)),
        ],
        compiler_params=pltpu.CompilerParams(collective_id=0, has_side_effects=True),
        name="expose",
    )(socs_weight, dose, threshold, pltpu.with_memory_space_constraint(mask, pltpu.VMEM), kernels, seam, *tables)
    final = jax.ShapeDtypeStruct((1, core // 2, core), jnp.float32)
    return pl.pallas_call(
        store_kernel,
        out_shape=(final, final),
        in_specs=[vmem, vmem],
        out_specs=(anywhere, anywhere),
        scratch_shapes=[pltpu.SemaphoreType.DMA((2,))],
        name="store",
    )(*(pltpu.with_memory_space_constraint(r, pltpu.VMEM) for r in results))


def solution(mesh):
    return jax.shard_map(
        on_device,
        mesh=mesh,
        in_specs=(
            P(("parts", "tile"), None, None),
            P("cond", None, None, None),
            P("cond", None),
            P("cond"),
            P("cond"),
        ),
        out_specs=(P(("parts", "tile"), "cond", None), P(("parts", "tile"), "cond", None)),
        check_vma=False,
    )
```

```python
import functools

import jax
import jax.numpy as jnp
import numpy as np
from jax import lax
from jax.experimental import pallas as pl
from jax.experimental.pallas import tpu as pltpu
from jax.sharding import PartitionSpec as P

MESH = pl.DeviceIdType.MESH
MARGIN = 64
BLUR = 8
LANES = 128
STEP = 3
PACK = 4
GROUP = 8

diffusion = 2.0
steepness = 8.0


def phase(pixels, pad_width, band_width):
    freq = np.arange(band_width) - band_width // 2
    angle = 2.0 * np.pi * ((pixels[:, None] * freq[None, :]) % pad_width) / pad_width
    return np.cos(angle), np.sin(angle)


def rounded_rows(exact):
    out = exact.astype(jnp.bfloat16).astype(np.float64)
    for row in out:
        for _ in range(64):
            excess = row.sum() - 1.0
            toward = np.full(row.shape, -np.inf if excess > 0 else np.inf).astype(jnp.bfloat16)
            moved = np.nextafter(row.astype(jnp.bfloat16), toward).astype(np.float64)
            left = np.abs(excess + moved - row)
            if excess == 0 or left.min() >= abs(excess):
                break
            row[left.argmin()] = moved[left.argmin()]
    return out


def make_tables(core, band_width):
    pad_width = core + 2 * MARGIN
    bf16 = lambda a: np.asarray(a, np.float32).astype(jnp.bfloat16)
    cos_in, sin_in = phase(np.arange(pad_width), pad_width, band_width)
    both = np.concatenate([cos_in, -sin_in], axis=1)
    columns = both[MARGIN : MARGIN + core]
    nil = np.zeros((MARGIN, 2 * band_width))
    strips = []
    for strip in (both[:MARGIN], both[MARGIN + core :]):
        strips.append(np.block([[strip, nil], [nil, strip]]))
    rows = np.concatenate([cos_in.T, sin_in.T], axis=0)
    own_rows = rows[:, MARGIN : MARGIN + core]
    far_rows = np.concatenate([rows[:, :MARGIN], rows[:, MARGIN + core :]], axis=1)
    count = pad_width // STEP
    cos_s, sin_s = phase(np.arange(count) * STEP, pad_width, band_width)
    first = np.block([[cos_s, -sin_s, -sin_s, cos_s], [sin_s, cos_s, cos_s, sin_s]])
    nil = np.zeros((band_width, count))
    second = np.block(
        [
            [cos_s.T, sin_s.T, nil, nil],
            [nil, nil, cos_s.T, sin_s.T],
            [-sin_s.T, cos_s.T, nil, nil],
            [nil, nil, -sin_s.T, cos_s.T],
        ]
    )
    offset = np.arange(core + 2 * BLUR)[None, :] - np.arange(core)[:, None] - BLUR
    taps = np.where(np.abs(offset) <= BLUR, np.exp(-(offset**2) / (2.0 * diffusion**2)), 0.0)
    reach = np.arange(-BLUR, BLUR + 1)
    taps = taps / np.sum(np.exp(-(reach**2) / (2.0 * diffusion**2)))
    pixel = np.arange(MARGIN - BLUR, MARGIN + core + BLUR)
    wave = np.arange(-(band_width - 1), band_width)
    apart = pixel[:, None] - STEP * np.arange(count)[None, :]
    interpolate = np.cos(2.0 * np.pi * apart[:, :, None] * wave / pad_width).sum(-1) / count
    smooth = taps @ interpolate
    smooth = rounded_rows(smooth)
    rows_out = np.concatenate([smooth, smooth], axis=1)
    cols_out = rows_out.T
    rows_out = rows_out.reshape(2, core // 2, 2 * count)
    return tuple(
        bf16(a) for a in (columns, np.stack(strips), own_rows, far_rows, first, second, rows_out, cols_out)
    )


def nt_dot(a, b):
    return lax.dot_general(a, b, (((1,), (1,)), ((), ())), preferred_element_type=jnp.float32)


def dot(a, b):
    return jnp.dot(a, b, preferred_element_type=jnp.float32)


def halves(a):
    high = a.astype(jnp.bfloat16)
    return high, (a - high.astype(jnp.float32)).astype(jnp.bfloat16)


def spot(tiles):
    grid_cols = min(8, tiles // 2)
    place = lax.rem(lax.axis_index("tile") + grid_cols // 2, tiles)
    column = lax.rem(place, grid_cols)
    row = lax.div(place, grid_cols)
    odd = lax.rem(row, 2) == 1
    seam_left = jnp.logical_and(odd, column == grid_cols // 2)
    seam_right = jnp.logical_and(odd, column == grid_cols // 2 - 1)
    return grid_cols, column, row, seam_left, seam_right


def last_columns(mask_v):
    rows, columns = mask_v.shape
    upper = mask_v[: rows // 2, columns - LANES :].astype(jnp.float32)
    lower = mask_v[rows // 2 :, columns - LANES :].astype(jnp.float32)
    early = lax.broadcasted_iota(jnp.int32, upper.shape, 1) < MARGIN
    return jnp.where(early, pltpu.roll(upper, MARGIN, axis=1), lower).astype(mask_v.dtype)


def first_columns(mask_v):
    rows = mask_v.shape[0]
    upper = mask_v[: rows // 2, :LANES].astype(jnp.float32)
    lower = mask_v[rows // 2 :, :LANES].astype(jnp.float32)
    early = lax.broadcasted_iota(jnp.int32, upper.shape, 1) < MARGIN
    return jnp.where(early, upper, pltpu.roll(lower, MARGIN, axis=1)).astype(mask_v.dtype)


def seam_kernel(tiles, mask_hbm, strip_hbm, mask_v, packed_v, load_sem, send_sem, recv_sem):
    tile = lax.axis_index("tile")
    _, _, _, seam_left, seam_right = spot(tiles)

    def exchange(peer, pack):
        barrier = pltpu.get_barrier_semaphore()
        pl.semaphore_signal(barrier, inc=1, device_id=peer, device_id_type=MESH)
        load = pltpu.make_async_copy(mask_hbm.at[0], mask_v, load_sem)
        load.start()
        load.wait()
        packed_v[...] = pack(mask_v)
        pl.semaphore_wait(barrier, 1)
        copy = pltpu.make_async_remote_copy(
            src_ref=packed_v,
            dst_ref=strip_hbm,
            send_sem=send_sem,
            recv_sem=recv_sem,
            device_id=peer,
            device_id_type=MESH,
        )
        copy.start()
        copy.wait()

    @pl.when(seam_right)
    def _():
        exchange({"tile": lax.rem(tile + 1, tiles)}, last_columns)

    @pl.when(seam_left)
    def _():
        exchange({"tile": lax.rem(tile + tiles - 1, tiles)}, first_columns)


def kernel(
    tiles,
    weight_hbm,
    dose_hbm,
    threshold_hbm,
    mask_ref,
    kernels_hbm,
    strip_hbm,
    columns_hbm,
    strips_hbm,
    own_rows_hbm,
    far_rows_hbm,
    first_hbm,
    second_hbm,
    rows_out_hbm,
    cols_out_hbm,
    high_ref,
    low_ref,
    weight_ref,
    dose_ref,
    threshold_ref,
    kernels_v,
    columns_v,
    strips_v,
    own_rows_v,
    far_rows_v,
    first_v,
    second_v,
    rows_out_v,
    cols_out_v,
    packed_v,
    left_v,
    right_v,
    spec_rows,
    far_v,
    pair_v,
    own_level,
    sib_level,
    load_sem,
    strip_sem,
    send_sem,
    recv_sem,
    level_send,
    level_recv,
):
    conds, kerns, band = kernels_v.shape[:3]
    mask_v = mask_ref.at[0]
    core = mask_v.shape[0]
    half = core // 2
    count = own_level.shape[1]
    tile = lax.axis_index("tile")
    cond = lax.axis_index("cond")
    grid_cols, column, row, seam_left, seam_right = spot(tiles)
    has_left = column > 0
    has_right = column < grid_cols - 1
    has_up = row > 0
    has_down = row < tiles // grid_cols - 1
    greet_left = jnp.logical_and(has_left, jnp.logical_not(seam_left))
    greet_right = jnp.logical_and(has_right, jnp.logical_not(seam_right))
    right = {"tile": lax.rem(tile + 1, tiles)}
    left = {"tile": lax.rem(tile + tiles - 1, tiles)}
    far = {"tile": lax.rem(tile + tiles + grid_cols * (2 * cond - 1), tiles), "cond": 1 - cond}
    far_row = row + 2 * cond - 1
    has_far = jnp.logical_and(far_row >= 0, far_row < tiles // grid_cols)
    other_row = row + 1 - 2 * cond
    has_other = jnp.logical_and(other_row >= 0, other_row < tiles // grid_cols)
    sibling = {"cond": 1 - cond}

    sources = (
        columns_hbm,
        strips_hbm,
        own_rows_hbm,
        far_rows_hbm,
        first_hbm,
        second_hbm,
        weight_hbm,
        dose_hbm,
        threshold_hbm,
        rows_out_hbm,
        cols_out_hbm,
        *[kernels_hbm.at[c] for c in range(conds)],
    )
    targets = (
        columns_v,
        strips_v,
        own_rows_v,
        far_rows_v,
        first_v,
        second_v,
        weight_ref,
        dose_ref,
        threshold_ref,
        rows_out_v,
        cols_out_v,
        *[kernels_v.at[c] for c in range(conds)],
    )
    loads = [
        pltpu.make_async_copy(s, t, load_sem.at[i]) for i, (s, t) in enumerate(zip(sources, targets))
    ]
    barrier = pltpu.get_barrier_semaphore()
    peers = 1
    for flag, peer in ((has_far, far), (greet_left, left), (greet_right, right)):
        peers = peers + flag.astype(jnp.int32)

        @pl.when(flag)
        def _(peer=peer):
            pl.semaphore_signal(barrier, inc=1, device_id=peer, device_id_type=MESH)

    pl.semaphore_signal(barrier, inc=1, device_id=sibling, device_id_type=MESH)
    from_seam = [
        (seam_left, pltpu.make_async_copy(strip_hbm, left_v, strip_sem)),
        (seam_right, pltpu.make_async_copy(strip_hbm, right_v, strip_sem)),
    ]
    for flag, copy in from_seam:
        pl.when(flag)(copy.start)

    def remote(src, dst, i, peer):
        return pltpu.make_async_remote_copy(
            src_ref=src,
            dst_ref=dst,
            send_sem=send_sem.at[i],
            recv_sem=recv_sem.at[i],
            device_id=peer,
            device_id_type=MESH,
        )

    to_right = remote(packed_v.at[0], left_v, 0, right)
    to_left = remote(packed_v.at[1], right_v, 1, left)
    edge = pl.ds(pl.multiple_of(cond * (core - MARGIN), MARGIN), MARGIN)
    to_far = remote(spec_rows.at[edge], far_v.at[1 - cond], 2, far)
    to_sibling = remote(far_v.at[cond], far_v.at[cond], 3, sibling)
    from_sibling = remote(far_v.at[1 - cond], far_v.at[1 - cond], 3, sibling)

    packed_v[0] = last_columns(mask_v)
    packed_v[1] = first_columns(mask_v)
    pl.semaphore_wait(barrier, peers)
    pl.when(greet_right)(to_right.start)
    pl.when(greet_left)(to_left.start)
    for load in loads:
        load.start()

    takes_first = jnp.logical_and(lax.rem(row, 2) == 0, column >= grid_cols // 2)
    hand_on_early = jnp.logical_and(has_far, takes_first)
    hand_on_late = jnp.logical_and(has_far, jnp.logical_not(takes_first))

    def hand_on():
        to_far.wait_recv()
        to_sibling.start()

    pl.when(hand_on_early)(hand_on)

    for load in loads:
        load.wait()
    part = dot(mask_v[...], columns_v[...])
    zero = jnp.zeros((half, LANES), jnp.bfloat16)
    pl.when(seam_left)(from_seam[0][1].wait)
    pl.when(seam_right)(from_seam[1][1].wait)
    pl.when(greet_left)(to_right.wait_recv)
    pl.when(greet_right)(to_left.wait_recv)
    aside = dot(jnp.where(has_left, left_v[...], zero), strips_v[0])
    aside += dot(jnp.where(has_right, right_v[...], zero), strips_v[1])
    spec_rows[:half] = (part[:half] + aside[:, : 2 * band]).astype(jnp.bfloat16)
    spec_rows[half:] = (part[half:] + aside[:, 2 * band :]).astype(jnp.bfloat16)
    pl.when(has_far)(to_far.start)
    mixed = dot(own_rows_v[...], spec_rows[...])

    pl.when(hand_on_late)(hand_on)
    pl.when(has_other)(from_sibling.wait_recv)
    zero = jnp.zeros((MARGIN, 2 * band), jnp.bfloat16)
    above = jnp.where(has_up, far_v[0], zero)
    below = jnp.where(has_down, far_v[1], zero)
    mixed += dot(far_rows_v[...], jnp.concatenate([above, below], axis=0))
    mixed *= 1.0 / ((core + 2 * MARGIN) * band)
    lower = lax.broadcasted_iota(jnp.int32, (band, 2 * band), 1) < band
    turned = pltpu.roll(mixed[band:], band, axis=1)
    spec = mixed[:band] + jnp.where(lower, turned, -turned)
    swapped = pltpu.roll(spec, band, axis=1)
    reals = jnp.where(lower, spec, swapped)
    imags = jnp.where(lower, swapped, -spec)

    steps = kerns // GROUP

    def first_half(s):
        c, g = divmod(s, steps)
        for i in range(GROUP // PACK):
            rows = []
            for j in range(PACK):
                held = kernels_v[c, g * GROUP + i * PACK + j].astype(jnp.float32)
                rows.append(
                    jnp.concatenate(
                        [(reals * held).astype(jnp.bfloat16), (imags * held).astype(jnp.bfloat16)],
                        axis=1,
                    )
                )
            out = nt_dot(first_v[...], jnp.concatenate(rows, axis=0)).astype(jnp.bfloat16)
            for j in range(PACK // 2):
                span = slice(j * 2 * band, (j + 1) * 2 * band)
                at = i * (PACK // 2) + j
                pair_v[s % 2, at * count : (at + 1) * count, : 2 * band] = out[:count, span]
                pair_v[s % 2, at * count : (at + 1) * count, 2 * band :] = out[count:, span]

    def second_half(s, level):
        c, g = divmod(s, steps)
        field = dot(pair_v[s % 2], second_v[...])
        for at in range(GROUP // 2):
            for i in range(2):
                re = field[at * count : (at + 1) * count, 2 * i * count : (2 * i + 1) * count]
                im = field[at * count : (at + 1) * count, (2 * i + 1) * count : (2 * i + 2) * count]
                term = weight_ref[c, g * GROUP + 2 * at + i] * (re * re + im * im)
                level = term if level is None else level + term
        return level

    rows_out = rows_out_v[cond]
    bounds = []

    def blur(levels):
        talls = []
        for level in levels:
            fine, rest = halves(level[...])
            tall = nt_dot(rows_out, jnp.concatenate([fine, rest], axis=1))
            talls.append(jnp.concatenate(halves(tall), axis=1))
        logits = dot(jnp.concatenate(talls, axis=0), cols_out_v[...])
        for i in range(len(levels)):
            logit = logits[i * half : (i + 1) * half]
            if bounds:
                bounds[0] = jnp.maximum(bounds[0], logit)
                bounds[1] = jnp.minimum(bounds[1], logit)
            else:
                bounds.extend([logit, logit])

    def finish(c, level):
        total = weight_ref[c, 0]
        for k in range(1, kerns):
            total += weight_ref[c, k]
        scale = jnp.full((1, count), steepness * dose_ref[c]) / jnp.full((1, count), total)
        own_level[c] = level * scale - steepness * threshold_ref[c]
        copy = pltpu.make_async_remote_copy(
            src_ref=own_level.at[c],
            dst_ref=sib_level.at[c],
            send_sem=level_send.at[c],
            recv_sem=level_recv.at[c],
            device_id=sibling,
            device_id_type=MESH,
        )
        copy.start()
        level_copies.append(copy)

    level_copies = []
    level = None
    levels = []
    first_half(0)
    for s in range(conds * steps):
        c = s // steps
        if s + 1 < conds * steps:
            first_half(s + 1)
        level = second_half(s, level)
        if s % steps == steps - 1:
            levels.append(level)
            level = None
            if c == conds - 2:
                for i in range(conds - 1):
                    finish(i, levels[i])
    finish(conds - 1, levels[-1])
    blur([own_level.at[c] for c in range(conds)])
    for copy in level_copies[:-1]:
        copy.wait_recv()
    blur([sib_level.at[c] for c in range(conds - 1)])
    level_copies[-1].wait_recv()
    blur([sib_level.at[conds - 1]])
    high_ref[0] = jax.nn.sigmoid(bounds[0])
    low_ref[0] = jax.nn.sigmoid(bounds[1])

    for flag, copy in (
        (greet_right, to_right),
        (greet_left, to_left),
        (has_far, to_far),
        (has_far, to_sibling),
    ):
        pl.when(flag)(copy.wait_send)
    for copy in level_copies:
        copy.wait_send()


def store_kernel(high_ref, low_ref, high_out, low_out, sem):
    copies = [
        pltpu.make_async_copy(high_ref, high_out, sem.at[0]),
        pltpu.make_async_copy(low_ref, low_out, sem.at[1]),
    ]
    for copy in copies:
        copy.start()
    for copy in copies:
        copy.wait()


def on_device(mask, kernels, socs_weight, dose, threshold):
    core = mask.shape[1]
    conds, kerns, band = kernels.shape[:3]
    tiles = lax.axis_size("tile")
    tables = [jnp.asarray(t) for t in make_tables(core, band)]
    count = (core + 2 * MARGIN) // STEP
    anywhere = pl.BlockSpec(memory_space=pl.ANY)
    vmem = pl.BlockSpec(memory_space=pltpu.VMEM)
    strip = (core // 2, LANES)
    seam = pl.pallas_call(
        functools.partial(seam_kernel, tiles),
        out_shape=jax.ShapeDtypeStruct(strip, mask.dtype),
        in_specs=[anywhere],
        out_specs=anywhere,
        scratch_shapes=[
            pltpu.VMEM(mask.shape[1:], mask.dtype),
            pltpu.VMEM(strip, mask.dtype),
            pltpu.SemaphoreType.DMA,
            pltpu.SemaphoreType.DMA,
            pltpu.SemaphoreType.DMA,
        ],
        compiler_params=pltpu.CompilerParams(collective_id=1, has_side_effects=True),
        cost_estimate=pl.CostEstimate(flops=10**9, bytes_accessed=4 * mask.size, transcendentals=0),
        name="seam",
    )(mask)
    loads = 3 + len(tables) + conds
    out = pltpu.VMEM((1, core // 2, core), jnp.float32)
    results = pl.pallas_call(
        functools.partial(kernel, tiles),
        out_shape=(out, out),
        in_specs=[anywhere] * 3 + [vmem] + [anywhere] * (2 + len(tables)),
        out_specs=(vmem, vmem),
        scratch_shapes=[
            *[pltpu.SMEM(a.shape, a.dtype) for a in (socs_weight, dose, threshold)],
            pltpu.VMEM(kernels.shape, kernels.dtype),
            *[pltpu.VMEM(t.shape, t.dtype) for t in tables],
            pltpu.VMEM((2, *strip), mask.dtype),
            pltpu.VMEM(strip, mask.dtype),
            pltpu.VMEM(strip, mask.dtype),
            pltpu.VMEM((core, 2 * band), jnp.bfloat16),
            pltpu.VMEM((2, MARGIN, 2 * band), jnp.bfloat16),
            pltpu.VMEM((2, GROUP // 2 * count, 4 * band), jnp.bfloat16),
            pltpu.VMEM((conds, count, count), jnp.float32),
            pltpu.VMEM((conds, count, count), jnp.float32),
            pltpu.SemaphoreType.DMA((loads,)),
            pltpu.SemaphoreType.DMA,
            pltpu.SemaphoreType.DMA((4,)),
            pltpu.SemaphoreType.DMA((4,)),
            pltpu.SemaphoreType.DMA((conds,)),
            pltpu.SemaphoreType.DMA((conds,)),
        ],
        compiler_params=pltpu.CompilerParams(collective_id=0, has_side_effects=True),
        name="expose",
    )(socs_weight, dose, threshold, pltpu.with_memory_space_constraint(mask, pltpu.VMEM), kernels, seam, *tables)
    final = jax.ShapeDtypeStruct((1, core // 2, core), jnp.float32)
    return pl.pallas_call(
        store_kernel,
        out_shape=(final, final),
        in_specs=[vmem, vmem],
        out_specs=(anywhere, anywhere),
        scratch_shapes=[pltpu.SemaphoreType.DMA((2,))],
        name="store",
    )(*(pltpu.with_memory_space_constraint(r, pltpu.VMEM) for r in results))


def solution(mesh):
    return jax.shard_map(
        on_device,
        mesh=mesh,
        in_specs=(
            P(("parts", "tile"), None, None),
            P("cond", None, None, None),
            P("cond", None),
            P("cond"),
            P("cond"),
        ),
        out_specs=(P(("parts", "tile"), "cond", None), P(("parts", "tile"), "cond", None)),
        check_vma=False,
    )
```

```python
import functools

import jax
import jax.numpy as jnp
import numpy as np
from jax import lax
from jax.experimental import pallas as pl
from jax.experimental.pallas import tpu as pltpu
from jax.sharding import PartitionSpec as P

MESH = pl.DeviceIdType.MESH
MARGIN = 64
BLUR = 8
LANES = 128
STEP = 3
PACK = 4
GROUP = 8

diffusion = 2.0
steepness = 8.0


def phase(pixels, pad_width, band_width):
    freq = np.arange(band_width) - band_width // 2
    angle = 2.0 * np.pi * ((pixels[:, None] * freq[None, :]) % pad_width) / pad_width
    return np.cos(angle), np.sin(angle)


def rounded_rows(exact):
    out = exact.astype(jnp.bfloat16).astype(np.float64)
    for row in out:
        for _ in range(64):
            excess = row.sum() - 1.0
            toward = np.full(row.shape, -np.inf if excess > 0 else np.inf).astype(jnp.bfloat16)
            moved = np.nextafter(row.astype(jnp.bfloat16), toward).astype(np.float64)
            left = np.abs(excess + moved - row)
            if excess == 0 or left.min() >= abs(excess):
                break
            row[left.argmin()] = moved[left.argmin()]
    return out


def make_tables(core, band_width):
    pad_width = core + 2 * MARGIN
    bf16 = lambda a: np.asarray(a, np.float32).astype(jnp.bfloat16)
    cos_in, sin_in = phase(np.arange(pad_width), pad_width, band_width)
    both = np.concatenate([cos_in, -sin_in], axis=1)
    columns = both[MARGIN : MARGIN + core]
    nil = np.zeros((MARGIN, 2 * band_width))
    strips = []
    for strip in (both[:MARGIN], both[MARGIN + core :]):
        strips.append(np.block([[strip, nil], [nil, strip]]))
    rows = np.concatenate([cos_in.T, sin_in.T], axis=0)
    own_rows = rows[:, MARGIN : MARGIN + core]
    far_rows = np.concatenate([rows[:, :MARGIN], rows[:, MARGIN + core :]], axis=1)
    count = pad_width // STEP
    cos_s, sin_s = phase(np.arange(count) * STEP, pad_width, band_width)
    first = np.block([[cos_s, -sin_s, -sin_s, cos_s], [sin_s, cos_s, cos_s, sin_s]])
    nil = np.zeros((band_width, count))
    second = np.block(
        [
            [cos_s.T, sin_s.T, nil, nil],
            [nil, nil, cos_s.T, sin_s.T],
            [-sin_s.T, cos_s.T, nil, nil],
            [nil, nil, -sin_s.T, cos_s.T],
        ]
    )
    offset = np.arange(core + 2 * BLUR)[None, :] - np.arange(core)[:, None] - BLUR
    taps = np.where(np.abs(offset) <= BLUR, np.exp(-(offset**2) / (2.0 * diffusion**2)), 0.0)
    reach = np.arange(-BLUR, BLUR + 1)
    taps = taps / np.sum(np.exp(-(reach**2) / (2.0 * diffusion**2)))
    pixel = np.arange(MARGIN - BLUR, MARGIN + core + BLUR)
    wave = np.arange(-(band_width - 1), band_width)
    apart = pixel[:, None] - STEP * np.arange(count)[None, :]
    interpolate = np.cos(2.0 * np.pi * apart[:, :, None] * wave / pad_width).sum(-1) / count
    smooth = taps @ interpolate
    smooth = rounded_rows(smooth)
    rows_out = np.concatenate([smooth, smooth], axis=1)
    cols_out = rows_out.T
    rows_out = rows_out.reshape(2, core // 2, 2 * count)
    return tuple(
        bf16(a) for a in (columns, np.stack(strips), own_rows, far_rows, first, second, rows_out, cols_out)
    )


def nt_dot(a, b):
    return lax.dot_general(a, b, (((1,), (1,)), ((), ())), preferred_element_type=jnp.float32)


def dot(a, b):
    return jnp.dot(a, b, preferred_element_type=jnp.float32)


def halves(a):
    high = a.astype(jnp.bfloat16)
    return high, (a - high.astype(jnp.float32)).astype(jnp.bfloat16)


def spot(tiles):
    grid_cols = min(8, tiles // 2)
    place = lax.rem(lax.axis_index("tile") + grid_cols // 2, tiles)
    column = lax.rem(place, grid_cols)
    row = lax.div(place, grid_cols)
    odd = lax.rem(row, 2) == 1
    seam_left = jnp.logical_and(odd, column == grid_cols // 2)
    seam_right = jnp.logical_and(odd, column == grid_cols // 2 - 1)
    return grid_cols, column, row, seam_left, seam_right


def last_columns(mask_v):
    rows, columns = mask_v.shape
    upper = mask_v[: rows // 2, columns - LANES :].astype(jnp.float32)
    lower = mask_v[rows // 2 :, columns - LANES :].astype(jnp.float32)
    early = lax.broadcasted_iota(jnp.int32, upper.shape, 1) < MARGIN
    return jnp.where(early, pltpu.roll(upper, MARGIN, axis=1), lower).astype(mask_v.dtype)


def first_columns(mask_v):
    rows = mask_v.shape[0]
    upper = mask_v[: rows // 2, :LANES].astype(jnp.float32)
    lower = mask_v[rows // 2 :, :LANES].astype(jnp.float32)
    early = lax.broadcasted_iota(jnp.int32, upper.shape, 1) < MARGIN
    return jnp.where(early, upper, pltpu.roll(lower, MARGIN, axis=1)).astype(mask_v.dtype)


def seam_kernel(tiles, mask_hbm, strip_hbm, mask_v, packed_v, load_sem, send_sem, recv_sem):
    tile = lax.axis_index("tile")
    _, _, _, seam_left, seam_right = spot(tiles)

    def exchange(peer, pack):
        barrier = pltpu.get_barrier_semaphore()
        pl.semaphore_signal(barrier, inc=1, device_id=peer, device_id_type=MESH)
        load = pltpu.make_async_copy(mask_hbm.at[0], mask_v, load_sem)
        load.start()
        load.wait()
        packed_v[...] = pack(mask_v)
        pl.semaphore_wait(barrier, 1)
        copy = pltpu.make_async_remote_copy(
            src_ref=packed_v,
            dst_ref=strip_hbm,
            send_sem=send_sem,
            recv_sem=recv_sem,
            device_id=peer,
            device_id_type=MESH,
        )
        copy.start()
        copy.wait()

    @pl.when(seam_right)
    def _():
        exchange({"tile": lax.rem(tile + 1, tiles)}, last_columns)

    @pl.when(seam_left)
    def _():
        exchange({"tile": lax.rem(tile + tiles - 1, tiles)}, first_columns)


def kernel(
    tiles,
    weight_hbm,
    dose_hbm,
    threshold_hbm,
    mask_ref,
    kernels_hbm,
    strip_hbm,
    columns_hbm,
    strips_hbm,
    own_rows_hbm,
    far_rows_hbm,
    first_hbm,
    second_hbm,
    rows_out_hbm,
    cols_out_hbm,
    high_ref,
    low_ref,
    weight_ref,
    dose_ref,
    threshold_ref,
    kernels_v,
    columns_v,
    strips_v,
    own_rows_v,
    far_rows_v,
    first_v,
    second_v,
    rows_out_v,
    cols_out_v,
    packed_v,
    left_v,
    right_v,
    spec_rows,
    far_v,
    pair_v,
    own_level,
    sib_level,
    load_sem,
    strip_sem,
    send_sem,
    recv_sem,
    level_send,
    level_recv,
):
    conds, kerns, band = kernels_v.shape[:3]
    mask_v = mask_ref.at[0]
    core = mask_v.shape[0]
    half = core // 2
    count = own_level.shape[1]
    tile = lax.axis_index("tile")
    cond = lax.axis_index("cond")
    grid_cols, column, row, seam_left, seam_right = spot(tiles)
    has_left = column > 0
    has_right = column < grid_cols - 1
    has_up = row > 0
    has_down = row < tiles // grid_cols - 1
    greet_left = jnp.logical_and(has_left, jnp.logical_not(seam_left))
    greet_right = jnp.logical_and(has_right, jnp.logical_not(seam_right))
    right_tile = lax.rem(tile + 1, tiles)
    left_tile = lax.rem(tile + tiles - 1, tiles)
    strips_out = cond == 1
    far = {"tile": lax.rem(tile + tiles + grid_cols * (2 * cond - 1), tiles), "cond": 1 - cond}
    far_row = row + 2 * cond - 1
    has_far = jnp.logical_and(far_row >= 0, far_row < tiles // grid_cols)
    other_row = row + 1 - 2 * cond
    has_other = jnp.logical_and(other_row >= 0, other_row < tiles // grid_cols)
    sibling = {"cond": 1 - cond}

    sources = (
        columns_hbm,
        strips_hbm,
        own_rows_hbm,
        far_rows_hbm,
        first_hbm,
        second_hbm,
        weight_hbm,
        dose_hbm,
        threshold_hbm,
        rows_out_hbm,
        cols_out_hbm,
        *[kernels_hbm.at[c] for c in range(conds)],
    )
    targets = (
        columns_v,
        strips_v,
        own_rows_v,
        far_rows_v,
        first_v,
        second_v,
        weight_ref,
        dose_ref,
        threshold_ref,
        rows_out_v,
        cols_out_v,
        *[kernels_v.at[c] for c in range(conds)],
    )
    loads = [
        pltpu.make_async_copy(s, t, load_sem.at[i]) for i, (s, t) in enumerate(zip(sources, targets))
    ]
    barrier = pltpu.get_barrier_semaphore()
    for flag, peer in (
        (greet_left, {"tile": left_tile, "cond": 1}),
        (greet_right, {"tile": right_tile, "cond": 1}),
        (has_far, far),
    ):

        @pl.when(flag)
        def _(peer=peer):
            pl.semaphore_signal(barrier, inc=1, device_id=peer, device_id_type=MESH)

    beside = greet_left.astype(jnp.int32) + greet_right.astype(jnp.int32)
    peers = 1 + has_far.astype(jnp.int32) + 2 * cond * beside
    pl.semaphore_signal(barrier, inc=1, device_id=sibling, device_id_type=MESH)
    from_seam = [
        (seam_left, pltpu.make_async_copy(strip_hbm, left_v, strip_sem)),
        (seam_right, pltpu.make_async_copy(strip_hbm, right_v, strip_sem)),
    ]
    for flag, copy in from_seam:
        pl.when(flag)(copy.start)

    def remote(src, dst, i, peer):
        return pltpu.make_async_remote_copy(
            src_ref=src,
            dst_ref=dst,
            send_sem=send_sem.at[i],
            recv_sem=recv_sem.at[i],
            device_id=peer,
            device_id_type=MESH,
        )

    to_right, to_left = [
        [
            pltpu.make_async_remote_copy(
                src_ref=packed_v.at[side],
                dst_ref=strip_v,
                send_sem=send_sem.at[4 + 2 * side + i],
                recv_sem=recv_sem.at[side],
                device_id={"tile": peer, "cond": i},
                device_id_type=MESH,
            )
            for i in range(2)
        ]
        for side, strip_v, peer in ((0, left_v, right_tile), (1, right_v, left_tile))
    ]
    from_left, from_right = to_right[0], to_left[0]
    send_right = jnp.logical_and(greet_right, strips_out)
    send_left = jnp.logical_and(greet_left, strips_out)
    edge = pl.ds(pl.multiple_of(cond * (core - MARGIN), MARGIN), MARGIN)
    to_far = remote(spec_rows.at[edge], far_v.at[1 - cond], 2, far)
    to_sibling = remote(far_v.at[cond], far_v.at[cond], 3, sibling)
    from_sibling = remote(far_v.at[1 - cond], far_v.at[1 - cond], 3, sibling)

    takes_first = jnp.logical_and(lax.rem(row, 2) == 0, column >= grid_cols // 2)

    def start_loads():
        for load in loads:
            load.start()

    pl.when(takes_first)(start_loads)
    packed_v[0] = last_columns(mask_v)
    pl.semaphore_wait(barrier, peers)
    for copy in to_right:
        pl.when(send_right)(copy.start)
    packed_v[1] = first_columns(mask_v)
    for copy in to_left:
        pl.when(send_left)(copy.start)
    pl.when(jnp.logical_not(takes_first))(start_loads)

    hand_on_early = jnp.logical_and(has_far, takes_first)
    hand_on_late = jnp.logical_and(has_far, jnp.logical_not(takes_first))

    def hand_on():
        to_far.wait_recv()
        to_sibling.start()

    pl.when(hand_on_early)(hand_on)

    for load in loads:
        load.wait()
    part = dot(mask_v[...], columns_v[...])
    zero = jnp.zeros((half, LANES), jnp.bfloat16)
    pl.when(seam_left)(from_seam[0][1].wait)
    pl.when(seam_right)(from_seam[1][1].wait)
    pl.when(greet_left)(from_left.wait_recv)
    pl.when(greet_right)(from_right.wait_recv)
    aside = dot(jnp.where(has_left, left_v[...], zero), strips_v[0])
    aside += dot(jnp.where(has_right, right_v[...], zero), strips_v[1])
    spec_rows[:half] = (part[:half] + aside[:, : 2 * band]).astype(jnp.bfloat16)
    spec_rows[half:] = (part[half:] + aside[:, 2 * band :]).astype(jnp.bfloat16)
    pl.when(has_far)(to_far.start)
    mixed = dot(own_rows_v[...], spec_rows[...])

    pl.when(hand_on_late)(hand_on)
    pl.when(has_other)(from_sibling.wait_recv)
    zero = jnp.zeros((MARGIN, 2 * band), jnp.bfloat16)
    above = jnp.where(has_up, far_v[0], zero)
    below = jnp.where(has_down, far_v[1], zero)
    mixed += dot(far_rows_v[...], jnp.concatenate([above, below], axis=0))
    mixed *= 1.0 / ((core + 2 * MARGIN) * band)
    lower = lax.broadcasted_iota(jnp.int32, (band, 2 * band), 1) < band
    turned = pltpu.roll(mixed[band:], band, axis=1)
    spec = mixed[:band] + jnp.where(lower, turned, -turned)
    swapped = pltpu.roll(spec, band, axis=1)
    reals = jnp.where(lower, spec, swapped)
    imags = jnp.where(lower, swapped, -spec)

    steps = kerns // GROUP

    def first_half(s):
        c, g = divmod(s, steps)
        for i in range(GROUP // PACK):
            rows = []
            for j in range(PACK):
                held = kernels_v[c, g * GROUP + i * PACK + j].astype(jnp.float32)
                rows.append(
                    jnp.concatenate(
                        [(reals * held).astype(jnp.bfloat16), (imags * held).astype(jnp.bfloat16)],
                        axis=1,
                    )
                )
            out = nt_dot(first_v[...], jnp.concatenate(rows, axis=0)).astype(jnp.bfloat16)
            for j in range(PACK // 2):
                span = slice(j * 2 * band, (j + 1) * 2 * band)
                at = i * (PACK // 2) + j
                pair_v[s % 2, at * count : (at + 1) * count, : 2 * band] = out[:count, span]
                pair_v[s % 2, at * count : (at + 1) * count, 2 * band :] = out[count:, span]

    def second_half(s, level):
        c, g = divmod(s, steps)
        field = dot(pair_v[s % 2], second_v[...])
        for at in range(GROUP // 2):
            for i in range(2):
                re = field[at * count : (at + 1) * count, 2 * i * count : (2 * i + 1) * count]
                im = field[at * count : (at + 1) * count, (2 * i + 1) * count : (2 * i + 2) * count]
                term = weight_ref[c, g * GROUP + 2 * at + i] * (re * re + im * im)
                level = term if level is None else level + term
        return level

    rows_out = rows_out_v[cond]
    bounds = []

    def blur(levels):
        talls = []
        for level in levels:
            fine, rest = halves(level[...])
            tall = nt_dot(rows_out, jnp.concatenate([fine, rest], axis=1))
            talls.append(jnp.concatenate(halves(tall), axis=1))
        logits = dot(jnp.concatenate(talls, axis=0), cols_out_v[...])
        for i in range(len(levels)):
            logit = logits[i * half : (i + 1) * half]
            if bounds:
                bounds[0] = jnp.maximum(bounds[0], logit)
                bounds[1] = jnp.minimum(bounds[1], logit)
            else:
                bounds.extend([logit, logit])

    def finish(c, level):
        total = weight_ref[c, 0]
        for k in range(1, kerns):
            total += weight_ref[c, k]
        scale = jnp.full((1, count), steepness * dose_ref[c]) / jnp.full((1, count), total)
        own_level[c] = level * scale - steepness * threshold_ref[c]
        copy = pltpu.make_async_remote_copy(
            src_ref=own_level.at[c],
            dst_ref=sib_level.at[c],
            send_sem=level_send.at[c],
            recv_sem=level_recv.at[c],
            device_id=sibling,
            device_id_type=MESH,
        )
        copy.start()
        level_copies.append(copy)

    level_copies = []
    level = None
    levels = []
    first_half(0)
    for s in range(conds * steps):
        c = s // steps
        if s + 1 < conds * steps:
            first_half(s + 1)
        level = second_half(s, level)
        if s % steps == steps - 1:
            levels.append(level)
            level = None
            if c == conds - 2:
                for i in range(conds - 1):
                    finish(i, levels[i])
    finish(conds - 1, levels[-1])
    blur([own_level.at[c] for c in range(conds)])
    for copy in level_copies[:-1]:
        copy.wait_recv()
    blur([sib_level.at[c] for c in range(conds - 1)])
    level_copies[-1].wait_recv()
    blur([sib_level.at[conds - 1]])
    high_ref[0] = jax.nn.sigmoid(bounds[0])
    low_ref[0] = jax.nn.sigmoid(bounds[1])

    for flag, copy in (
        (send_right, to_right[0]),
        (send_right, to_right[1]),
        (send_left, to_left[0]),
        (send_left, to_left[1]),
        (has_far, to_far),
        (has_far, to_sibling),
    ):
        pl.when(flag)(copy.wait_send)
    for copy in level_copies:
        copy.wait_send()


def store_kernel(high_ref, low_ref, high_out, low_out, sem):
    copies = [
        pltpu.make_async_copy(high_ref, high_out, sem.at[0]),
        pltpu.make_async_copy(low_ref, low_out, sem.at[1]),
    ]
    for copy in copies:
        copy.start()
    for copy in copies:
        copy.wait()


def on_device(mask, kernels, socs_weight, dose, threshold):
    core = mask.shape[1]
    conds, kerns, band = kernels.shape[:3]
    tiles = lax.axis_size("tile")
    tables = [jnp.asarray(t) for t in make_tables(core, band)]
    count = (core + 2 * MARGIN) // STEP
    anywhere = pl.BlockSpec(memory_space=pl.ANY)
    vmem = pl.BlockSpec(memory_space=pltpu.VMEM)
    strip = (core // 2, LANES)
    seam = pl.pallas_call(
        functools.partial(seam_kernel, tiles),
        out_shape=jax.ShapeDtypeStruct(strip, mask.dtype),
        in_specs=[anywhere],
        out_specs=anywhere,
        scratch_shapes=[
            pltpu.VMEM(mask.shape[1:], mask.dtype),
            pltpu.VMEM(strip, mask.dtype),
            pltpu.SemaphoreType.DMA,
            pltpu.SemaphoreType.DMA,
            pltpu.SemaphoreType.DMA,
        ],
        compiler_params=pltpu.CompilerParams(collective_id=1, has_side_effects=True),
        cost_estimate=pl.CostEstimate(flops=10**9, bytes_accessed=4 * mask.size, transcendentals=0),
        name="seam",
    )(mask)
    loads = 3 + len(tables) + conds
    out = pltpu.VMEM((1, core // 2, core), jnp.float32)
    results = pl.pallas_call(
        functools.partial(kernel, tiles),
        out_shape=(out, out),
        in_specs=[anywhere] * 3 + [vmem] + [anywhere] * (2 + len(tables)),
        out_specs=(vmem, vmem),
        scratch_shapes=[
            *[pltpu.SMEM(a.shape, a.dtype) for a in (socs_weight, dose, threshold)],
            pltpu.VMEM(kernels.shape, kernels.dtype),
            *[pltpu.VMEM(t.shape, t.dtype) for t in tables],
            pltpu.VMEM((2, *strip), mask.dtype),
            pltpu.VMEM(strip, mask.dtype),
            pltpu.VMEM(strip, mask.dtype),
            pltpu.VMEM((core, 2 * band), jnp.bfloat16),
            pltpu.VMEM((2, MARGIN, 2 * band), jnp.bfloat16),
            pltpu.VMEM((2, GROUP // 2 * count, 4 * band), jnp.bfloat16),
            pltpu.VMEM((conds, count, count), jnp.float32),
            pltpu.VMEM((conds, count, count), jnp.float32),
            pltpu.SemaphoreType.DMA((loads,)),
            pltpu.SemaphoreType.DMA,
            pltpu.SemaphoreType.DMA((8,)),
            pltpu.SemaphoreType.DMA((4,)),
            pltpu.SemaphoreType.DMA((conds,)),
            pltpu.SemaphoreType.DMA((conds,)),
        ],
        compiler_params=pltpu.CompilerParams(collective_id=0, has_side_effects=True),
        name="expose",
    )(socs_weight, dose, threshold, pltpu.with_memory_space_constraint(mask, pltpu.VMEM), kernels, seam, *tables)
    final = jax.ShapeDtypeStruct((1, core // 2, core), jnp.float32)
    return pl.pallas_call(
        store_kernel,
        out_shape=(final, final),
        in_specs=[vmem, vmem],
        out_specs=(anywhere, anywhere),
        scratch_shapes=[pltpu.SemaphoreType.DMA((2,))],
        name="store",
    )(*(pltpu.with_memory_space_constraint(r, pltpu.VMEM) for r in results))


def solution(mesh):
    return jax.shard_map(
        on_device,
        mesh=mesh,
        in_specs=(
            P(("parts", "tile"), None, None),
            P("cond", None, None, None),
            P("cond", None),
            P("cond"),
            P("cond"),
        ),
        out_specs=(P(("parts", "tile"), "cond", None), P(("parts", "tile"), "cond", None)),
        check_vma=False,
    )
```

```python
import functools

import jax
import jax.numpy as jnp
import numpy as np
from jax import lax
from jax.experimental import pallas as pl
from jax.experimental.pallas import tpu as pltpu
from jax.sharding import PartitionSpec as P

MESH = pl.DeviceIdType.MESH
MARGIN = 64
BLUR = 8
LANES = 128
STEP = 3
PACK = 4
GROUP = 8

diffusion = 2.0
steepness = 8.0


def phase(pixels, pad_width, band_width):
    freq = np.arange(band_width) - band_width // 2
    angle = 2.0 * np.pi * ((pixels[:, None] * freq[None, :]) % pad_width) / pad_width
    return np.cos(angle), np.sin(angle)


def rounded_rows(exact):
    out = exact.astype(jnp.bfloat16).astype(np.float64)
    for row in out:
        for _ in range(64):
            excess = row.sum() - 1.0
            toward = np.full(row.shape, -np.inf if excess > 0 else np.inf).astype(jnp.bfloat16)
            moved = np.nextafter(row.astype(jnp.bfloat16), toward).astype(np.float64)
            left = np.abs(excess + moved - row)
            if excess == 0 or left.min() >= abs(excess):
                break
            row[left.argmin()] = moved[left.argmin()]
    return out


def make_tables(core, band_width):
    pad_width = core + 2 * MARGIN
    bf16 = lambda a: np.asarray(a, np.float32).astype(jnp.bfloat16)
    cos_in, sin_in = phase(np.arange(pad_width), pad_width, band_width)
    both = np.concatenate([cos_in, -sin_in], axis=1)
    columns = both[MARGIN : MARGIN + core]
    nil = np.zeros((MARGIN, 2 * band_width))
    strips = []
    for strip in (both[:MARGIN], both[MARGIN + core :]):
        strips.append(np.block([[strip, nil], [nil, strip]]))
    rows = np.concatenate([cos_in.T, sin_in.T], axis=0)
    own_rows = rows[:, MARGIN : MARGIN + core]
    far_rows = np.concatenate([rows[:, :MARGIN], rows[:, MARGIN + core :]], axis=1)
    count = pad_width // STEP
    cos_s, sin_s = phase(np.arange(count) * STEP, pad_width, band_width)
    first = np.block([[cos_s, -sin_s, -sin_s, cos_s], [sin_s, cos_s, cos_s, sin_s]])
    nil = np.zeros((band_width, count))
    second = np.block(
        [
            [cos_s.T, sin_s.T, nil, nil],
            [nil, nil, cos_s.T, sin_s.T],
            [-sin_s.T, cos_s.T, nil, nil],
            [nil, nil, -sin_s.T, cos_s.T],
        ]
    )
    offset = np.arange(core + 2 * BLUR)[None, :] - np.arange(core)[:, None] - BLUR
    taps = np.where(np.abs(offset) <= BLUR, np.exp(-(offset**2) / (2.0 * diffusion**2)), 0.0)
    reach = np.arange(-BLUR, BLUR + 1)
    taps = taps / np.sum(np.exp(-(reach**2) / (2.0 * diffusion**2)))
    pixel = np.arange(MARGIN - BLUR, MARGIN + core + BLUR)
    wave = np.arange(-(band_width - 1), band_width)
    apart = pixel[:, None] - STEP * np.arange(count)[None, :]
    interpolate = np.cos(2.0 * np.pi * apart[:, :, None] * wave / pad_width).sum(-1) / count
    smooth = taps @ interpolate
    smooth = rounded_rows(smooth)
    rows_out = np.concatenate([smooth, smooth], axis=1)
    cols_out = rows_out.T
    rows_out = rows_out.reshape(2, core // 2, 2 * count)
    return tuple(
        bf16(a) for a in (columns, np.stack(strips), own_rows, far_rows, first, second, rows_out, cols_out)
    )


def nt_dot(a, b):
    return lax.dot_general(a, b, (((1,), (1,)), ((), ())), preferred_element_type=jnp.float32)


def dot(a, b):
    return jnp.dot(a, b, preferred_element_type=jnp.float32)


def halves(a):
    high = a.astype(jnp.bfloat16)
    return high, (a - high.astype(jnp.float32)).astype(jnp.bfloat16)


def spot(tiles):
    grid_cols = min(8, tiles // 2)
    place = lax.rem(lax.axis_index("tile") + grid_cols // 2, tiles)
    column = lax.rem(place, grid_cols)
    row = lax.div(place, grid_cols)
    odd = lax.rem(row, 2) == 1
    seam_left = jnp.logical_and(odd, column == grid_cols // 2)
    seam_right = jnp.logical_and(odd, column == grid_cols // 2 - 1)
    return grid_cols, column, row, seam_left, seam_right


def last_columns(mask_v):
    rows, columns = mask_v.shape
    upper = mask_v[: rows // 2, columns - LANES :].astype(jnp.float32)
    lower = mask_v[rows // 2 :, columns - LANES :].astype(jnp.float32)
    early = lax.broadcasted_iota(jnp.int32, upper.shape, 1) < MARGIN
    return jnp.where(early, pltpu.roll(upper, MARGIN, axis=1), lower).astype(mask_v.dtype)


def first_columns(mask_v):
    rows = mask_v.shape[0]
    upper = mask_v[: rows // 2, :LANES].astype(jnp.float32)
    lower = mask_v[rows // 2 :, :LANES].astype(jnp.float32)
    early = lax.broadcasted_iota(jnp.int32, upper.shape, 1) < MARGIN
    return jnp.where(early, upper, pltpu.roll(lower, MARGIN, axis=1)).astype(mask_v.dtype)


def seam_kernel(tiles, mask_hbm, strip_hbm, mask_v, packed_v, load_sem, send_sem, recv_sem):
    tile = lax.axis_index("tile")
    _, _, _, seam_left, seam_right = spot(tiles)

    def exchange(peer, pack):
        barrier = pltpu.get_barrier_semaphore()
        pl.semaphore_signal(barrier, inc=1, device_id=peer, device_id_type=MESH)
        load = pltpu.make_async_copy(mask_hbm.at[0], mask_v, load_sem)
        load.start()
        load.wait()
        packed_v[...] = pack(mask_v)
        pl.semaphore_wait(barrier, 1)
        copy = pltpu.make_async_remote_copy(
            src_ref=packed_v,
            dst_ref=strip_hbm,
            send_sem=send_sem,
            recv_sem=recv_sem,
            device_id=peer,
            device_id_type=MESH,
        )
        copy.start()
        copy.wait()

    @pl.when(seam_right)
    def _():
        exchange({"tile": lax.rem(tile + 1, tiles)}, last_columns)

    @pl.when(seam_left)
    def _():
        exchange({"tile": lax.rem(tile + tiles - 1, tiles)}, first_columns)


def kernel(
    tiles,
    weight_hbm,
    dose_hbm,
    threshold_hbm,
    mask_ref,
    kernels_hbm,
    strip_hbm,
    columns_hbm,
    strips_hbm,
    own_rows_hbm,
    far_rows_hbm,
    first_hbm,
    second_hbm,
    rows_out_hbm,
    cols_out_hbm,
    high_ref,
    low_ref,
    weight_ref,
    dose_ref,
    threshold_ref,
    kernels_v,
    columns_v,
    strips_v,
    own_rows_v,
    far_rows_v,
    first_v,
    second_v,
    rows_out_v,
    cols_out_v,
    packed_v,
    left_v,
    right_v,
    spec_rows,
    far_v,
    pair_v,
    own_level,
    sib_level,
    load_sem,
    strip_sem,
    send_sem,
    recv_sem,
    level_send,
    level_recv,
):
    conds, kerns, band = kernels_v.shape[:3]
    mask_v = mask_ref.at[0]
    core = mask_v.shape[0]
    half = core // 2
    count = own_level.shape[1]
    tile = lax.axis_index("tile")
    cond = lax.axis_index("cond")
    grid_cols, column, row, seam_left, seam_right = spot(tiles)
    has_left = column > 0
    has_right = column < grid_cols - 1
    has_up = row > 0
    has_down = row < tiles // grid_cols - 1
    greet_left = jnp.logical_and(has_left, jnp.logical_not(seam_left))
    greet_right = jnp.logical_and(has_right, jnp.logical_not(seam_right))
    right_tile = lax.rem(tile + 1, tiles)
    left_tile = lax.rem(tile + tiles - 1, tiles)
    strips_out = cond == 1
    far = {"tile": lax.rem(tile + tiles + grid_cols * (2 * cond - 1), tiles), "cond": 1 - cond}
    far_row = row + 2 * cond - 1
    has_far = jnp.logical_and(far_row >= 0, far_row < tiles // grid_cols)
    other_row = row + 1 - 2 * cond
    has_other = jnp.logical_and(other_row >= 0, other_row < tiles // grid_cols)
    sibling = {"cond": 1 - cond}

    sources = (
        columns_hbm,
        strips_hbm,
        own_rows_hbm,
        far_rows_hbm,
        first_hbm,
        second_hbm,
        weight_hbm,
        dose_hbm,
        threshold_hbm,
        rows_out_hbm,
        cols_out_hbm,
        *[kernels_hbm.at[c] for c in range(conds)],
    )
    targets = (
        columns_v,
        strips_v,
        own_rows_v,
        far_rows_v,
        first_v,
        second_v,
        weight_ref,
        dose_ref,
        threshold_ref,
        rows_out_v,
        cols_out_v,
        *[kernels_v.at[c] for c in range(conds)],
    )
    loads = [
        pltpu.make_async_copy(s, t, load_sem.at[i]) for i, (s, t) in enumerate(zip(sources, targets))
    ]
    barrier = pltpu.get_barrier_semaphore()
    pl.semaphore_signal(barrier, inc=1, device_id=sibling, device_id_type=MESH)
    for flag, peer in (
        (greet_left, {"tile": left_tile, "cond": 1}),
        (greet_right, {"tile": right_tile, "cond": 1}),
        (has_far, far),
    ):

        @pl.when(flag)
        def _(peer=peer):
            pl.semaphore_signal(barrier, inc=1, device_id=peer, device_id_type=MESH)

    beside = greet_left.astype(jnp.int32) + greet_right.astype(jnp.int32)
    peers = 1 + has_far.astype(jnp.int32) + 2 * cond * beside
    from_seam = [
        (seam_left, pltpu.make_async_copy(strip_hbm, left_v, strip_sem)),
        (seam_right, pltpu.make_async_copy(strip_hbm, right_v, strip_sem)),
    ]
    for flag, copy in from_seam:
        pl.when(flag)(copy.start)

    def remote(src, dst, i, peer):
        return pltpu.make_async_remote_copy(
            src_ref=src,
            dst_ref=dst,
            send_sem=send_sem.at[i],
            recv_sem=recv_sem.at[i],
            device_id=peer,
            device_id_type=MESH,
        )

    to_right, to_left = [
        [
            pltpu.make_async_remote_copy(
                src_ref=packed_v.at[side],
                dst_ref=strip_v,
                send_sem=send_sem.at[4 + 2 * side + i],
                recv_sem=recv_sem.at[side],
                device_id={"tile": peer, "cond": i},
                device_id_type=MESH,
            )
            for i in range(2)
        ]
        for side, strip_v, peer in ((0, left_v, right_tile), (1, right_v, left_tile))
    ]
    from_left, from_right = to_right[0], to_left[0]
    send_right = jnp.logical_and(greet_right, strips_out)
    send_left = jnp.logical_and(greet_left, strips_out)
    edge = pl.ds(pl.multiple_of(cond * (core - MARGIN), MARGIN), MARGIN)
    to_far = remote(spec_rows.at[edge], far_v.at[1 - cond], 2, far)
    to_sibling = remote(far_v.at[cond], far_v.at[cond], 3, sibling)
    from_sibling = remote(far_v.at[1 - cond], far_v.at[1 - cond], 3, sibling)

    takes_first = jnp.logical_and(lax.rem(row, 2) == 0, column >= grid_cols // 2)

    def start_loads():
        for load in loads:
            load.start()

    pl.when(takes_first)(start_loads)
    packed_v[0] = last_columns(mask_v)
    pl.semaphore_wait(barrier, peers)
    for copy in to_right:
        pl.when(send_right)(copy.start)
    packed_v[1] = first_columns(mask_v)
    for copy in to_left:
        pl.when(send_left)(copy.start)
    pl.when(jnp.logical_not(takes_first))(start_loads)

    hand_on_early = jnp.logical_and(has_far, takes_first)
    hand_on_late = jnp.logical_and(has_far, jnp.logical_not(takes_first))

    def hand_on():
        to_far.wait_recv()
        to_sibling.start()

    pl.when(hand_on_early)(hand_on)

    for load in loads:
        load.wait()
    part = dot(mask_v[...], columns_v[...])
    zero = jnp.zeros((half, LANES), jnp.bfloat16)
    pl.when(seam_left)(from_seam[0][1].wait)
    pl.when(seam_right)(from_seam[1][1].wait)
    pl.when(greet_left)(from_left.wait_recv)
    pl.when(greet_right)(from_right.wait_recv)
    aside = dot(jnp.where(has_left, left_v[...], zero), strips_v[0])
    aside += dot(jnp.where(has_right, right_v[...], zero), strips_v[1])
    spec_rows[:half] = (part[:half] + aside[:, : 2 * band]).astype(jnp.bfloat16)
    spec_rows[half:] = (part[half:] + aside[:, 2 * band :]).astype(jnp.bfloat16)
    pl.when(has_far)(to_far.start)
    mixed = dot(own_rows_v[...], spec_rows[...])

    pl.when(hand_on_late)(hand_on)
    pl.when(has_other)(from_sibling.wait_recv)
    zero = jnp.zeros((MARGIN, 2 * band), jnp.bfloat16)
    above = jnp.where(has_up, far_v[0], zero)
    below = jnp.where(has_down, far_v[1], zero)
    mixed += dot(far_rows_v[...], jnp.concatenate([above, below], axis=0))
    mixed *= 1.0 / ((core + 2 * MARGIN) * band)
    lower = lax.broadcasted_iota(jnp.int32, (band, 2 * band), 1) < band
    turned = pltpu.roll(mixed[band:], band, axis=1)
    spec = mixed[:band] + jnp.where(lower, turned, -turned)
    swapped = pltpu.roll(spec, band, axis=1)
    reals = jnp.where(lower, spec, swapped)
    imags = jnp.where(lower, swapped, -spec)

    steps = kerns // GROUP

    def first_half(s):
        c, g = divmod(s, steps)
        for i in range(GROUP // PACK):
            rows = []
            for j in range(PACK):
                held = kernels_v[c, g * GROUP + i * PACK + j].astype(jnp.float32)
                rows.append(
                    jnp.concatenate(
                        [(reals * held).astype(jnp.bfloat16), (imags * held).astype(jnp.bfloat16)],
                        axis=1,
                    )
                )
            out = nt_dot(first_v[...], jnp.concatenate(rows, axis=0)).astype(jnp.bfloat16)
            for j in range(PACK // 2):
                span = slice(j * 2 * band, (j + 1) * 2 * band)
                at = i * (PACK // 2) + j
                pair_v[s % 2, at * count : (at + 1) * count, : 2 * band] = out[:count, span]
                pair_v[s % 2, at * count : (at + 1) * count, 2 * band :] = out[count:, span]

    def second_half(s, level):
        c, g = divmod(s, steps)
        field = dot(pair_v[s % 2], second_v[...])
        for at in range(GROUP // 2):
            for i in range(2):
                re = field[at * count : (at + 1) * count, 2 * i * count : (2 * i + 1) * count]
                im = field[at * count : (at + 1) * count, (2 * i + 1) * count : (2 * i + 2) * count]
                term = weight_ref[c, g * GROUP + 2 * at + i] * (re * re + im * im)
                level = term if level is None else level + term
        return level

    rows_out = rows_out_v[cond]
    bounds = []

    def blur(levels):
        talls = []
        for level in levels:
            fine, rest = halves(level[...])
            tall = nt_dot(rows_out, jnp.concatenate([fine, rest], axis=1))
            talls.append(jnp.concatenate(halves(tall), axis=1))
        logits = dot(jnp.concatenate(talls, axis=0), cols_out_v[...])
        for i in range(len(levels)):
            logit = logits[i * half : (i + 1) * half]
            if bounds:
                bounds[0] = jnp.maximum(bounds[0], logit)
                bounds[1] = jnp.minimum(bounds[1], logit)
            else:
                bounds.extend([logit, logit])

    def finish(c, level):
        total = weight_ref[c, 0]
        for k in range(1, kerns):
            total += weight_ref[c, k]
        scale = jnp.full((1, count), steepness * dose_ref[c]) / jnp.full((1, count), total)
        own_level[c] = level * scale - steepness * threshold_ref[c]
        copy = pltpu.make_async_remote_copy(
            src_ref=own_level.at[c],
            dst_ref=sib_level.at[c],
            send_sem=level_send.at[c],
            recv_sem=level_recv.at[c],
            device_id=sibling,
            device_id_type=MESH,
        )
        copy.start()
        level_copies.append(copy)

    level_copies = []
    level = None
    levels = []
    first_half(0)
    for s in range(conds * steps):
        c = s // steps
        if s + 1 < conds * steps:
            first_half(s + 1)
        if s == (conds - 1) * steps:
            for i in range(conds - 1):
                finish(i, levels[i])
        level = second_half(s, level)
        if s % steps == steps - 1:
            levels.append(level)
            level = None
    finish(conds - 1, levels[-1])
    blur([own_level.at[c] for c in range(conds)])
    for copy in level_copies[:-1]:
        copy.wait_recv()
    blur([sib_level.at[c] for c in range(conds - 1)])
    level_copies[-1].wait_recv()
    blur([sib_level.at[conds - 1]])
    high_ref[0] = jax.nn.sigmoid(bounds[0])
    low_ref[0] = jax.nn.sigmoid(bounds[1])

    for flag, copy in (
        (send_right, to_right[0]),
        (send_right, to_right[1]),
        (send_left, to_left[0]),
        (send_left, to_left[1]),
        (has_far, to_far),
        (has_far, to_sibling),
    ):
        pl.when(flag)(copy.wait_send)
    for copy in level_copies:
        copy.wait_send()


def store_kernel(high_ref, low_ref, high_out, low_out, sem):
    copies = [
        pltpu.make_async_copy(high_ref, high_out, sem.at[0]),
        pltpu.make_async_copy(low_ref, low_out, sem.at[1]),
    ]
    for copy in copies:
        copy.start()
    for copy in copies:
        copy.wait()


def on_device(mask, kernels, socs_weight, dose, threshold):
    core = mask.shape[1]
    conds, kerns, band = kernels.shape[:3]
    tiles = lax.axis_size("tile")
    tables = [jnp.asarray(t) for t in make_tables(core, band)]
    count = (core + 2 * MARGIN) // STEP
    anywhere = pl.BlockSpec(memory_space=pl.ANY)
    vmem = pl.BlockSpec(memory_space=pltpu.VMEM)
    strip = (core // 2, LANES)
    seam = pl.pallas_call(
        functools.partial(seam_kernel, tiles),
        out_shape=jax.ShapeDtypeStruct(strip, mask.dtype),
        in_specs=[anywhere],
        out_specs=anywhere,
        scratch_shapes=[
            pltpu.VMEM(mask.shape[1:], mask.dtype),
            pltpu.VMEM(strip, mask.dtype),
            pltpu.SemaphoreType.DMA,
            pltpu.SemaphoreType.DMA,
            pltpu.SemaphoreType.DMA,
        ],
        compiler_params=pltpu.CompilerParams(collective_id=1, has_side_effects=True),
        cost_estimate=pl.CostEstimate(flops=10**9, bytes_accessed=4 * mask.size, transcendentals=0),
        name="seam",
    )(mask)
    loads = 3 + len(tables) + conds
    out = pltpu.VMEM((1, core // 2, core), jnp.float32)
    results = pl.pallas_call(
        functools.partial(kernel, tiles),
        out_shape=(out, out),
        in_specs=[anywhere] * 3 + [vmem] + [anywhere] * (2 + len(tables)),
        out_specs=(vmem, vmem),
        scratch_shapes=[
            *[pltpu.SMEM(a.shape, a.dtype) for a in (socs_weight, dose, threshold)],
            pltpu.VMEM(kernels.shape, kernels.dtype),
            *[pltpu.VMEM(t.shape, t.dtype) for t in tables],
            pltpu.VMEM((2, *strip), mask.dtype),
            pltpu.VMEM(strip, mask.dtype),
            pltpu.VMEM(strip, mask.dtype),
            pltpu.VMEM((core, 2 * band), jnp.bfloat16),
            pltpu.VMEM((2, MARGIN, 2 * band), jnp.bfloat16),
            pltpu.VMEM((2, GROUP // 2 * count, 4 * band), jnp.bfloat16),
            pltpu.VMEM((conds, count, count), jnp.float32),
            pltpu.VMEM((conds, count, count), jnp.float32),
            pltpu.SemaphoreType.DMA((loads,)),
            pltpu.SemaphoreType.DMA,
            pltpu.SemaphoreType.DMA((8,)),
            pltpu.SemaphoreType.DMA((4,)),
            pltpu.SemaphoreType.DMA((conds,)),
            pltpu.SemaphoreType.DMA((conds,)),
        ],
        compiler_params=pltpu.CompilerParams(collective_id=0, has_side_effects=True),
        name="expose",
    )(socs_weight, dose, threshold, pltpu.with_memory_space_constraint(mask, pltpu.VMEM), kernels, seam, *tables)
    final = jax.ShapeDtypeStruct((1, core // 2, core), jnp.float32)
    return pl.pallas_call(
        store_kernel,
        out_shape=(final, final),
        in_specs=[vmem, vmem],
        out_specs=(anywhere, anywhere),
        scratch_shapes=[pltpu.SemaphoreType.DMA((2,))],
        name="store",
    )(*(pltpu.with_memory_space_constraint(r, pltpu.VMEM) for r in results))


def solution(mesh):
    return jax.shard_map(
        on_device,
        mesh=mesh,
        in_specs=(
            P(("parts", "tile"), None, None),
            P("cond", None, None, None),
            P("cond", None),
            P("cond"),
            P("cond"),
        ),
        out_specs=(P(("parts", "tile"), "cond", None), P(("parts", "tile"), "cond", None)),
        check_vma=False,
    )
```
